8 devices in a mesh: rep: 2 (over y, z), dp: 4 (over x, core).
Axes of the slice: x: 2, y: 2, z: 1, core: 2. Of those that a mesh axis runs over, the one named last changes fastest.
Arguments:
- x: bfloat16 [8, 2048, 512], P(('rep', 'dp')), parts along dimension 0
- dy: bfloat16 [8, 2048, 512], P(('rep', 'dp')), parts along dimension 0
- w_gate: bfloat16 [2, 512, 8192], replicated
- w_up: bfloat16 [2, 512, 8192], replicated
- w_down: bfloat16 [2, 8192, 512], replicated
- m_w_gate: float32 [2, 512, 8192], P(None, 'dp')
- m_w_up: float32 [2, 512, 8192], P(None, 'dp')
- m_w_down: float32 [2, 8192, 512], P(None, 'dp')
- v_w_gate: float32 [2, 512, 8192], P(None, 'dp')
- v_w_up: float32 [2, 512, 8192], P(None, 'dp')
- v_w_down: float32 [2, 8192, 512], P(None, 'dp')
Outputs:
- output 1: bfloat16 [4, 512, 8192], P('rep'), parts along dimension 0
- output 2: bfloat16 [4, 512, 8192], P('rep'), parts along dimension 0
- output 3: bfloat16 [4, 8192, 512], P('rep'), parts along dimension 0
- output 4: float32 [4, 512, 8192], P('rep', 'dp'), parts along dimension 0
- output 5: float32 [4, 512, 8192], P('rep', 'dp'), parts along dimension 0
- output 6: float32 [4, 8192, 512], P('rep', 'dp'), parts along dimension 0
- output 7: float32 [4, 512, 8192], P('rep', 'dp'), parts along dimension 0
- output 8: float32 [4, 512, 8192], P('rep', 'dp'), parts along dimension 0
- output 9: float32 [4, 8192, 512], P('rep', 'dp'), parts along dimension 0
There are 2 independent parts. The reference program is written for one: setup_inputs(seed, part) draws one part's arguments, and reference() takes and returns one part's arrays. A program takes and returns all parts, laid end to end along the dimension named above; an argument that names none is the same for every part.
All inputs are finite; a program needn't handle non-finite values.
Results may differ from the reference program's by a relative error of at most 0.022.
Values are sent between devices in bfloat16 or wider.
A program may use at most 2 GiB of HBM per device.

```python
import jax
import jax.numpy as jnp
from jax import lax

SEQUENCES = 4
TOKENS = 2048
D = 512
FF = 8192
LAYERS = 2
NAMES = ("w_gate", "w_up", "w_down")
SHAPES = {"w_gate": (LAYERS, D, FF), "w_up": (LAYERS, D, FF), "w_down": (LAYERS, FF, D)}


def bump(key, n, height):
    away = (jnp.arange(n, dtype=jnp.int32) - jax.random.randint(key, (), 0, n, jnp.int32)) % n
    return jnp.where(away < n // 8, height, 1.0)


def together(key, own, strength):
    shared = jax.random.normal(key, own.shape[1:], jnp.float32)
    return (own + strength * shared) * lax.rsqrt(1 + strength * strength)


def setup_inputs(seed: int = 0, part: int = 0) -> dict:
    kx, kdy, ka, kb, kz, kf, kh, kl, *keys = jax.random.split(jax.random.key(seed), 8 + 3 * len(NAMES))
    kx, kdy, ka, kb = (jax.random.fold_in(k, part) for k in (kx, kdy, ka, kb))
    kw, km, kv = (keys[i::3] for i in range(3))
    shape = (SEQUENCES, TOKENS, D)
    much_x, much_dy = jax.random.uniform(kz, (2,), jnp.float32, 0.0, 1.0)
    loud = 2.0 ** jax.random.uniform(jax.random.fold_in(kz, 1), (), jnp.float32, -1.0, 2.0)
    layers = 2.0 ** jax.random.uniform(kl, (LAYERS, 1, 1), jnp.float32, -1.0, 1.0)
    x = together(ka, jax.random.normal(kx, shape, jnp.float32), much_x) * bump(kf, D, 4.0)
    dy = together(kb, jax.random.normal(kdy, shape, jnp.float32), much_dy)
    drawn = {"x": x.astype(jnp.bfloat16), "dy": (loud * dy * (SEQUENCES * TOKENS) ** -0.5).astype(jnp.bfloat16)}
    for key, name in zip(kw, NAMES, strict=True):
        w = jax.random.normal(key, SHAPES[name], jnp.float32) * SHAPES[name][1] ** -0.5
        drawn[name] = (w * {"w_gate": 1.0, "w_up": bump(kh, FF, 4.0), "w_down": layers}[name]).astype(jnp.bfloat16)
    for key, name in zip(km, NAMES, strict=True):
        drawn[f"m_{name}"] = 0.1 * jax.random.normal(key, SHAPES[name], jnp.float32)
    for key, name in zip(kv, NAMES, strict=True):
        drawn[f"v_{name}"] = jax.random.uniform(key, SHAPES[name], jnp.float32, 0.005, 0.015)
    return drawn


def matmul(a, w):
    return jnp.dot(a, w, preferred_element_type=jnp.float32).astype(jnp.bfloat16)


def normed(h):
    wide = h.astype(jnp.float32)
    scale = lax.rsqrt(jnp.mean(wide**2, -1, keepdims=True) + 1e-6)
    return (wide * scale).astype(jnp.bfloat16)


def layer(h, w):
    a = normed(h)
    gate = jnp.dot(a, w["w_gate"], preferred_element_type=jnp.float32)
    up = jnp.dot(a, w["w_up"], preferred_element_type=jnp.float32)
    return h + matmul((jax.nn.silu(gate) * up).astype(jnp.bfloat16), w["w_down"])


def adamw(w, m, v, g):
    m = 0.9 * m + 0.1 * g
    v = 0.95 * v + 0.05 * g * g
    step = m * lax.rsqrt(v + 1e-8) + 0.1 * w
    return (w - 0.02 * step).astype(jnp.bfloat16), m, v


def clipped(gradients, sum_of_squares, count):
    factor = jnp.minimum(1.0, 0.5 * lax.rsqrt(sum_of_squares / count + 1e-30))
    return [g * factor for g in gradients]


def stack(weights, h):
    return lax.scan(lambda h, w: (layer(h, w), None), h, weights)[0]


def reference(x, dy, w_gate, w_up, w_down, m_w_gate, m_w_up, m_w_down, v_w_gate, v_w_up, v_w_down):
    weights = dict(zip(NAMES, (w_gate, w_up, w_down), strict=True))

    def take(so_far, sequence):
        h, by_y = sequence
        _, back = jax.vjp(lambda w: stack(w, h), weights)
        return jax.tree.map(lambda total, term: total + term.astype(jnp.float32), so_far, back(by_y)[0]), None

    none_yet = {name: jnp.zeros(w.shape, jnp.float32) for name, w in weights.items()}
    by_weights, _ = lax.scan(take, none_yet, (x, dy))
    gradients = [by_weights[name].astype(jnp.bfloat16).astype(jnp.float32) for name in NAMES]
    gradients = clipped(gradients, sum(jnp.sum(g * g) for g in gradients), sum(g.size for g in gradients))
    new = [
        adamw(w.astype(jnp.float32), m, v, g)
        for w, m, v, g in zip((w_gate, w_up, w_down), (m_w_gate, m_w_up, m_w_down), (v_w_gate, v_w_up, v_w_down), gradients, strict=True)
    ]
    return tuple(one[which] for which in range(3) for one in new)
```

```python
import functools

import jax
import jax.numpy as jnp
from jax import lax
from jax.experimental import pallas as pl
from jax.experimental.pallas import tpu as pltpu
from jax.sharding import PartitionSpec as P

F32, BF16 = jnp.float32, jnp.bfloat16
TOKENS, D, FF = 2048, 512, 8192
LAYERS, DP = 2, 4
CHUNKS = 4
OWN = FF // DP
TILE = OWN // CHUNKS
ROWS = D // DP
COUNT = 3 * LAYERS * D * FF
VMEM = 60 * 1024 * 1024


def dot(a, b):
    return jnp.dot(a, b, preferred_element_type=F32)


def dot_nt(a, b):
    return lax.dot_general(a, b, (((1,), (1,)), ((), ())), preferred_element_type=F32)


def sigmoid(x):
    return 0.5 * jnp.tanh(0.5 * x) + 0.5


def normed(h):
    wide = h.astype(F32)
    return (wide * lax.rsqrt(jnp.mean(wide * wide, -1, keepdims=True) + 1e-6)).astype(BF16)


def flipped(t):
    return t.astype(F32).T.astype(BF16)


def whole(shape):
    return pl.BlockSpec(shape, lambda *_: (0,) * len(shape), pipeline_mode=pl.Buffered(1))


def params(n):
    return pltpu.CompilerParams(dimension_semantics=("arbitrary",) * n, vmem_limit_bytes=VMEM)


def cost(units, moved):
    return pl.CostEstimate(flops=int(units * 2 * TOKENS * D * FF), bytes_accessed=int(moved), transcendentals=0)


FT, FI = 1024, 1024


def forward_kernel(x_ref, dy_ref, wg_ref, wu_ref, wd_ref, h1_ref, a0_ref, a1_ref, a0t_ref, a1t_ref, dyt_ref, acc_ref, z_ref):
    j, i = pl.program_id(0), pl.program_id(1)
    rows = pl.ds(pl.multiple_of(i * FI, FI), FI)

    @pl.when(j == 0)
    def _():
        a = normed(x_ref[rows, :])
        a0_ref[rows, :] = a
        a0t_ref[:, rows] = flipped(a)
        dyt_ref[:, rows] = flipped(dy_ref[rows, :])
        acc_ref[rows, :] = jnp.zeros((FI, D), F32)

    a = a0_ref[rows, :]
    for s in range(0, FT, 256):
        gate = dot(a, wg_ref[0, :, s : s + 256])
        up = dot(a, wu_ref[0, :, s : s + 256])
        z_ref[:, s : s + 256] = (gate * sigmoid(gate) * up).astype(BF16)
    acc_ref[rows, :] += dot(z_ref[...], wd_ref[0])

    @pl.when(j == FF // FT - 1)
    def _():
        h1 = x_ref[rows, :] + acc_ref[rows, :].astype(BF16)
        a1 = normed(h1)
        h1_ref[rows, :] = h1
        a1_ref[rows, :] = a1
        a1t_ref[:, rows] = flipped(a1)


def forward(x, dy, wg, wu, wd):
    row, col = jax.ShapeDtypeStruct((TOKENS, D), BF16), jax.ShapeDtypeStruct((D, TOKENS), BF16)
    return pl.pallas_call(
        forward_kernel,
        grid=(FF // FT, TOKENS // FI),
        in_specs=[
            whole((TOKENS, D)),
            whole((TOKENS, D)),
            pl.BlockSpec((1, D, FT), lambda j, i: (0, 0, j)),
            pl.BlockSpec((1, D, FT), lambda j, i: (0, 0, j)),
            pl.BlockSpec((1, FT, D), lambda j, i: (0, j, 0)),
        ],
        out_specs=[whole((TOKENS, D))] * 3 + [whole((D, TOKENS))] * 3,
        out_shape=[row] * 3 + [col] * 3,
        scratch_shapes=[pltpu.VMEM((TOKENS, D), F32), pltpu.VMEM((FI, FT), BF16)],
        compiler_params=params(2),
        cost_estimate=cost(3, 40e6),
        name="forward0",
    )(x, dy, wg, wu, wd)


BI = 1024


def backward_kernel(with_da, me_ref, a_ref, at_ref, dy_ref, dyt_ref, wg_ref, wu_ref, wd_ref, own_gu, far_gu, give_gu, own_d, far_d, give_d, *rest):
    if with_da:
        da_ref, *rest = rest
    acc_g, acc_u, acc_d, z_ref, dg_ref, du_ref = rest
    r, i = pl.program_id(0), pl.program_id(1)
    me = me_ref[0]
    rows = pl.ds(pl.multiple_of(i * BI, BI), BI)
    a, dy = a_ref[rows, :], dy_ref[rows, :]
    for s in range(0, TILE, 256):
        c = slice(s, s + 256)
        gate = dot(a, wg_ref[0, :, c])
        up = dot(a, wu_ref[0, :, c])
        dz = dot_nt(dy, wd_ref[0, c, :]).astype(BF16).astype(F32)
        sig = sigmoid(gate)
        act = gate * sig
        z_ref[:, c] = (act * up).astype(BF16)
        du_ref[:, c] = (dz * act).astype(BF16)
        dg_ref[:, c] = (dz * up * (sig + act * (1.0 - sig))).astype(BF16)

    @pl.when(i == 0)
    def _():
        for acc in (acc_g, acc_u, acc_d):
            acc[...] = jnp.zeros((D, TILE), F32)

    if with_da:

        @pl.when(r == 0)
        def _():
            da_ref[rows, :] = jnp.zeros((BI, D), F32)

    acc_g[...] += dot(at_ref[:, rows], dg_ref[...])
    acc_u[...] += dot(at_ref[:, rows], du_ref[...])
    acc_d[...] += dot(dyt_ref[:, rows], z_ref[...])
    if with_da:
        da_ref[rows, :] += dot_nt(dg_ref[...], wg_ref[0]) + dot_nt(du_ref[...], wu_ref[0])

    @pl.when(i == TOKENS // BI - 1)
    def _():
        for k, acc in enumerate((acc_g, acc_u)):
            for q, to in enumerate((own_gu.at[k], give_gu.at[0, k], far_gu.at[k], give_gu.at[1, k])):
                to[...] = acc[pl.ds(pl.multiple_of((me ^ q) * ROWS, ROWS), ROWS), :].astype(BF16)
        for q, to in enumerate((own_d, give_d.at[0], far_d, give_d.at[1])):

            @pl.when(r == q)
            def _(to=to):
                to[...] = acc_d[...].T.astype(BF16)


def backward(layer, chunk, with_da, me, a, at, dy, dyt, wg, wu, wd):
    gu, d = jax.ShapeDtypeStruct((2, ROWS, OWN), BF16), jax.ShapeDtypeStruct((TILE, D), BF16)
    two_gu, two_d = jax.ShapeDtypeStruct((2, 2, ROWS, OWN), BF16), jax.ShapeDtypeStruct((2, TILE, D), BF16)

    def piece(r, me):
        return (r ^ me[0]) * CHUNKS + chunk

    gu_spec = pl.BlockSpec((2, ROWS, TILE), lambda r, i, me: (0, 0, r ^ me[0]))
    outs = [gu, gu, two_gu, d, d, two_d]
    out_specs = [
        gu_spec,
        gu_spec,
        pl.BlockSpec((2, 2, ROWS, TILE), lambda r, i, me: (0, 0, 0, r ^ me[0])),
        whole((TILE, D)),
        whole((TILE, D)),
        whole((2, TILE, D)),
    ]
    if with_da:
        outs.append(jax.ShapeDtypeStruct((TOKENS, D), F32))
        out_specs.append(whole((TOKENS, D)))
    return pl.pallas_call(
        functools.partial(backward_kernel, with_da),
        grid_spec=pltpu.PrefetchScalarGridSpec(
            num_scalar_prefetch=1,
            grid=(DP, TOKENS // BI),
            in_specs=[
                whole((TOKENS, D)),
                whole((D, TOKENS)),
                whole((TOKENS, D)),
                whole((D, TOKENS)),
                pl.BlockSpec((1, D, TILE), lambda r, i, me: (layer, 0, piece(r, me))),
                pl.BlockSpec((1, D, TILE), lambda r, i, me: (layer, 0, piece(r, me))),
                pl.BlockSpec((1, TILE, D), lambda r, i, me: (layer, piece(r, me), 0)),
            ],
            out_specs=out_specs,
            scratch_shapes=[pltpu.VMEM((D, TILE), F32)] * 3 + [pltpu.VMEM((BI, TILE), BF16)] * 3,
        ),
        out_shape=outs,
        compiler_params=params(2),
        cost_estimate=cost((8 if with_da else 6) / CHUNKS, 30e6),
        name=f"backward{layer}",
    )(me, a, at, dy, dyt, wg, wu, wd)


CI = 512


def between_kernel(h_ref, dy_ref, *refs):
    *parts, out_ref, outt_ref = refs
    da = parts[0][...]
    for part in parts[1:]:
        da = da + part[...]
    da = da.astype(BF16).astype(F32)
    wide = h_ref[...].astype(F32)
    scale = lax.rsqrt(jnp.mean(wide * wide, -1, keepdims=True) + 1e-6)
    dot_h = jnp.mean(da * wide, -1, keepdims=True)
    dh = (da * scale - wide * (scale * scale * scale * dot_h)).astype(BF16)
    dh = dy_ref[...] + dh
    out_ref[...] = dh
    outt_ref[...] = flipped(dh)


def between(h, dy, parts):
    block = pl.BlockSpec((CI, D), lambda i: (i, 0))
    return pl.pallas_call(
        between_kernel,
        grid=(TOKENS // CI,),
        in_specs=[block] * (2 + len(parts)),
        out_specs=[block, pl.BlockSpec((D, CI), lambda i: (0, i))],
        out_shape=[jax.ShapeDtypeStruct((TOKENS, D), BF16), jax.ShapeDtypeStruct((D, TOKENS), BF16)],
        compiler_params=params(1),
        cost_estimate=cost(0.4, 26e6),
        name="between",
    )(h, dy, *parts)


def adamw_kernel(me_ref, f_ref, ggu, gd, wg, wu, wd, mg, mu, md, vg, vu, vd, *refs):
    ngu, nd, *mv = refs[-8:]
    factor = f_ref[0, 0]
    for k, (g, w, m, v, to) in enumerate(
        (
            (ggu.at[0], wg.at[0], mg.at[0], vg.at[0], ngu.at[0]),
            (ggu.at[1], wu.at[0], mu.at[0], vu.at[0], ngu.at[1]),
            (gd, wd.at[0], md.at[0], vd.at[0], nd),
        )
    ):
        g = g[...].astype(F32) * factor
        m = 0.9 * m[...] + 0.1 * g
        v = 0.95 * v[...] + 0.05 * g * g
        w = w[...].astype(F32)
        to[...] = (w - 0.02 * (m * lax.rsqrt(v + 1e-8) + 0.1 * w)).astype(BF16)
        mv[k][0] = m
        mv[3 + k][0] = v


def adamw(layer, chunk, me, factor, ggu, gd, weights, m, v, so_far):
    step = TILE // DP
    w_spec = pl.BlockSpec((1, ROWS, TILE), lambda o, me: (layer, me[0], o * CHUNKS + chunk))
    wd_spec = pl.BlockSpec((1, step, D), lambda o, me: (layer, (me[0] * CHUNKS + chunk) * DP + o, 0))
    mv_spec = pl.BlockSpec((1, ROWS, TILE), lambda o, me: (layer, 0, o * CHUNKS + chunk))
    mvd_spec = pl.BlockSpec((1, step, D), lambda o, me: (layer, chunk * DP + o, 0))
    gu_spec = pl.BlockSpec((2, ROWS, TILE), lambda o, me: (0, 0, o))
    d_spec = pl.BlockSpec((step, D), lambda o, me: (o, 0))
    mv_specs = [mv_spec, mv_spec, mvd_spec] * 2
    return pl.pallas_call(
        adamw_kernel,
        grid_spec=pltpu.PrefetchScalarGridSpec(
            num_scalar_prefetch=1,
            grid=(DP,),
            in_specs=[pl.BlockSpec(memory_space=pltpu.SMEM), gu_spec, d_spec, w_spec, w_spec, wd_spec, *mv_specs]
            + [pl.BlockSpec(memory_space=pl.ANY)] * len(so_far),
            out_specs=[gu_spec, d_spec, *mv_specs],
        ),
        out_shape=[jax.ShapeDtypeStruct((2, ROWS, OWN), BF16), jax.ShapeDtypeStruct((TILE, D), BF16)]
        + [jax.ShapeDtypeStruct(t.shape, F32) for t in (*m, *v)],
        input_output_aliases={13 + n: 2 + n for n in range(len(so_far))},
        compiler_params=params(1),
        cost_estimate=cost(0.25, 17e6),
        name="adamw",
    )(me, factor, ggu, gd, *weights, *m, *v, *so_far)


def assemble_kernel(me_ref, gu0, d0, gu1, d1, *refs):
    wg, wu, wd = refs[-3:]
    for q, (gu, d) in enumerate(((gu0, d0), (gu1, d1))):

        @pl.when(pl.program_id(0) == q)
        def _(gu=gu, d=d):
            wg[0] = gu[0]
            wu[0] = gu[1]
            wd[0] = d[...]


def assemble(layer, chunk, base, me, first, second, so_far):
    step = TILE // DP

    def when(q, r, o):
        return jnp.where(r == q, o, 0 if q else DP - 1)

    def gu_spec(q):
        return pl.BlockSpec((2, ROWS, TILE), lambda r, o, me: (0, 0, when(q, r, o)))

    def d_spec(q):
        return pl.BlockSpec((step, D), lambda r, o, me: (when(q, r, o), 0))

    def owner(r, me):
        return (r + base) ^ me[0]

    w_spec = pl.BlockSpec((1, ROWS, TILE), lambda r, o, me: (layer, owner(r, me), o * CHUNKS + chunk))
    wd_spec = pl.BlockSpec((1, step, D), lambda r, o, me: (layer, (owner(r, me) * CHUNKS + chunk) * DP + o, 0))
    wide, tall = jax.ShapeDtypeStruct((LAYERS, D, FF), BF16), jax.ShapeDtypeStruct((LAYERS, FF, D), BF16)
    return pl.pallas_call(
        assemble_kernel,
        grid_spec=pltpu.PrefetchScalarGridSpec(
            num_scalar_prefetch=1,
            grid=(2, DP),
            in_specs=[gu_spec(0), d_spec(0), gu_spec(1), d_spec(1)] + [pl.BlockSpec(memory_space=pl.ANY)] * len(so_far),
            out_specs=[w_spec, w_spec, wd_spec],
        ),
        out_shape=[wide, wide, tall],
        input_output_aliases={5 + n: n for n in range(len(so_far))},
        compiler_params=params(2),
        cost_estimate=cost(0.15, 6e6),
        name="assemble",
    )(me, *first, *second, *so_far)


def to_core(t):
    return lax.ppermute(t, "dp", [(0, 1), (1, 0), (2, 3), (3, 2)])


def to_x(t):
    return lax.ppermute(t, "dp", [(0, 2), (2, 0), (1, 3), (3, 1)])


def solution(mesh):
    def body(x, dy, *arrays):
        weights, m, v = (arrays[i : i + 3] for i in (0, 3, 6))
        x, dy = x[0], dy[0]
        me = lax.axis_index("dp").astype(jnp.int32)[None]

        h1, a0, a1, a0t, a1t, dyt = forward(x, dy, *weights)

        gradients = {}

        def reduced(layer, chunk, parts):
            own_gu, far_gu, give_gu, own_d, far_d, give_d = parts
            got_gu, got_d = to_core(give_gu), to_core(give_d)
            sum_gu = (far_gu.astype(F32) + got_gu[1].astype(F32)).astype(BF16)
            sum_d = (far_d.astype(F32) + got_d[1].astype(F32)).astype(BF16)
            sum_gu, sum_d = to_x(sum_gu), to_x(sum_d)
            gu = (own_gu.astype(F32) + got_gu[0].astype(F32) + sum_gu.astype(F32)).astype(BF16)
            d = (own_d.astype(F32) + got_d[0].astype(F32) + sum_d.astype(F32)).astype(BF16)
            squares = jnp.sum(jnp.square(gu.astype(F32))) + jnp.sum(jnp.square(d.astype(F32)))
            gradients[layer, chunk] = gu, d, squares

        da = []
        for chunk in range(CHUNKS):
            *parts, part = backward(1, chunk, True, me, a1, a1t, dy, dyt, *weights)
            da.append(part)
            reduced(1, chunk, parts)
        dh, dht = between(h1, dy, da)
        for chunk in range(CHUNKS):
            reduced(0, chunk, backward(0, chunk, False, me, a0, a0t, dh, dht, *weights))

        total = lax.psum(sum(g[2] for g in gradients.values()), "dp")
        factor = jnp.minimum(1.0, 0.5 * lax.rsqrt(total / COUNT + 1e-30)).reshape(1, 1)

        moments, new = (), ()
        for (layer, chunk), (gu, d, _) in gradients.items():
            own_gu, own_d, *moments = adamw(layer, chunk, me, factor, gu, d, weights, m, v, moments)
            own = own_gu, own_d
            near = tuple(map(to_core, own))
            far = tuple(map(to_x, own))
            last = tuple(map(to_core, far))
            new = assemble(layer, chunk, 0, me, own, near, new)
            new = assemble(layer, chunk, 2, me, far, last, new)
        return (*new, *moments)

    rows = P(None, "dp", None)
    return jax.shard_map(
        body,
        mesh=mesh,
        in_specs=(P(("rep", "dp"), None, None),) * 2 + (P(None, None, None),) * 3 + (rows,) * 6,
        out_specs=(P("rep", None, None),) * 3 + (P("rep", "dp", None),) * 6,
        check_vma=False,
    )
```

```python
import functools

import jax
import jax.numpy as jnp
from jax import lax
from jax.experimental import pallas as pl
from jax.experimental.pallas import tpu as pltpu
from jax.sharding import PartitionSpec as P


F32, BF16 = jnp.float32, jnp.bfloat16
TOKENS, D, FF = 2048, 512, 8192
LAYERS, DP = 2, 4
CHUNKS = 4
OWN = FF // DP
TILE = OWN // CHUNKS
ROWS = D // DP
COUNT = 3 * LAYERS * D * FF
VMEM = 60 * 1024 * 1024


def dot(a, b):
    return jnp.dot(a, b, preferred_element_type=F32)


def dot_nt(a, b):
    return lax.dot_general(a, b, (((1,), (1,)), ((), ())), preferred_element_type=F32)


def sigmoid(x):
    return 0.5 * jnp.tanh(0.5 * x) + 0.5


def normed(h):
    wide = h.astype(F32)
    return (wide * lax.rsqrt(jnp.mean(wide * wide, -1, keepdims=True) + 1e-6)).astype(BF16)


def flipped(t):
    return t.astype(F32).T.astype(BF16)


def whole(shape):
    return pl.BlockSpec(shape, lambda *_: (0,) * len(shape), pipeline_mode=pl.Buffered(1))


def params(n):
    return pltpu.CompilerParams(dimension_semantics=("arbitrary",) * n, vmem_limit_bytes=VMEM)


def cost(units, moved):
    return pl.CostEstimate(flops=int(units * 2 * TOKENS * D * FF), bytes_accessed=int(moved), transcendentals=0)


FT, FI = 1024, 1024


def forward_kernel(x_ref, dy_ref, wg_ref, wu_ref, wd_ref, h1_ref, a0_ref, a1_ref, a0t_ref, a1t_ref, dyt_ref, acc_ref, z_ref):
    j, i = pl.program_id(0), pl.program_id(1)
    rows = pl.ds(pl.multiple_of(i * FI, FI), FI)

    @pl.when(j == 0)
    def _():
        a = normed(x_ref[rows, :])
        a0_ref[rows, :] = a
        a0t_ref[:, rows] = flipped(a)
        dyt_ref[:, rows] = flipped(dy_ref[rows, :])
        acc_ref[rows, :] = jnp.zeros((FI, D), F32)

    a = a0_ref[rows, :]
    for s in range(0, FT, 256):
        gate = dot(a, wg_ref[0, :, s : s + 256])
        up = dot(a, wu_ref[0, :, s : s + 256])
        z_ref[:, s : s + 256] = (gate * sigmoid(gate) * up).astype(BF16)
    acc_ref[rows, :] += dot(z_ref[...], wd_ref[0])

    @pl.when(j == FF // FT - 1)
    def _():
        h1 = x_ref[rows, :] + acc_ref[rows, :].astype(BF16)
        a1 = normed(h1)
        h1_ref[rows, :] = h1
        a1_ref[rows, :] = a1
        a1t_ref[:, rows] = flipped(a1)


def forward(x, dy, wg, wu, wd):
    row, col = jax.ShapeDtypeStruct((TOKENS, D), BF16), jax.ShapeDtypeStruct((D, TOKENS), BF16)
    return pl.pallas_call(
        forward_kernel,
        grid=(FF // FT, TOKENS // FI),
        in_specs=[
            whole((TOKENS, D)),
            whole((TOKENS, D)),
            pl.BlockSpec((1, D, FT), lambda j, i: (0, 0, j)),
            pl.BlockSpec((1, D, FT), lambda j, i: (0, 0, j)),
            pl.BlockSpec((1, FT, D), lambda j, i: (0, j, 0)),
        ],
        out_specs=[whole((TOKENS, D))] * 3 + [whole((D, TOKENS))] * 3,
        out_shape=[row] * 3 + [col] * 3,
        scratch_shapes=[pltpu.VMEM((TOKENS, D), F32), pltpu.VMEM((FI, FT), BF16)],
        compiler_params=params(2),
        cost_estimate=cost(3, 40e6),
        name="forward0",
    )(x, dy, wg, wu, wd)


BI = 1024


def backward_kernel(with_da, me_ref, a_ref, at_ref, dy_ref, dyt_ref, wg_ref, wu_ref, wd_ref, own_gu, far_gu, give_gu, own_d, far_d, give_d, *rest):
    if with_da:
        da_ref, *rest = rest
    acc_g, acc_u, acc_d, z_ref, dg_ref, du_ref = rest
    r, i = pl.program_id(0), pl.program_id(1)
    me = me_ref[0]
    rows = pl.ds(pl.multiple_of(i * BI, BI), BI)
    a, dy = a_ref[rows, :], dy_ref[rows, :]
    for s in range(0, TILE, 256):
        c = slice(s, s + 256)
        gate = dot(a, wg_ref[0, :, c])
        up = dot(a, wu_ref[0, :, c])
        dz = dot_nt(dy, wd_ref[0, c, :]).astype(BF16).astype(F32)
        sig = sigmoid(gate)
        act = gate * sig
        z_ref[:, c] = (act * up).astype(BF16)
        du_ref[:, c] = (dz * act).astype(BF16)
        dg_ref[:, c] = (dz * up * (sig + act * (1.0 - sig))).astype(BF16)

    @pl.when(i == 0)
    def _():
        for acc in (acc_g, acc_u, acc_d):
            acc[...] = jnp.zeros((D, TILE), F32)

    if with_da:

        @pl.when(r == 0)
        def _():
            da_ref[rows, :] = jnp.zeros((BI, D), F32)

    acc_g[...] += dot(at_ref[:, rows], dg_ref[...])
    acc_u[...] += dot(at_ref[:, rows], du_ref[...])
    acc_d[...] += dot(dyt_ref[:, rows], z_ref[...])
    if with_da:
        da_ref[rows, :] += dot_nt(dg_ref[...], wg_ref[0]) + dot_nt(du_ref[...], wu_ref[0])

    @pl.when(i == TOKENS // BI - 1)
    def _():
        for k, acc in enumerate((acc_g, acc_u)):
            for q, to in enumerate((own_gu.at[k], give_gu.at[0, k], far_gu.at[k], give_gu.at[1, k])):
                to[...] = acc[pl.ds(pl.multiple_of((me ^ q) * ROWS, ROWS), ROWS), :].astype(BF16)
        for q, to in enumerate((own_d, give_d.at[0], far_d, give_d.at[1])):

            @pl.when(r == q)
            def _(to=to):
                to[...] = acc_d[...].T.astype(BF16)


def backward(layer, chunk, with_da, me, a, at, dy, dyt, wg, wu, wd):
    gu, d = jax.ShapeDtypeStruct((2, ROWS, OWN), BF16), jax.ShapeDtypeStruct((TILE, D), BF16)
    two_gu, two_d = jax.ShapeDtypeStruct((2, 2, ROWS, OWN), BF16), jax.ShapeDtypeStruct((2, TILE, D), BF16)

    def piece(r, me):
        return (r ^ me[0]) * CHUNKS + chunk

    gu_spec = pl.BlockSpec((2, ROWS, TILE), lambda r, i, me: (0, 0, r ^ me[0]))
    outs = [gu, gu, two_gu, d, d, two_d]
    out_specs = [
        gu_spec,
        gu_spec,
        pl.BlockSpec((2, 2, ROWS, TILE), lambda r, i, me: (0, 0, 0, r ^ me[0])),
        whole((TILE, D)),
        whole((TILE, D)),
        whole((2, TILE, D)),
    ]
    if with_da:
        outs.append(jax.ShapeDtypeStruct((TOKENS, D), F32))
        out_specs.append(whole((TOKENS, D)))
    return pl.pallas_call(
        functools.partial(backward_kernel, with_da),
        grid_spec=pltpu.PrefetchScalarGridSpec(
            num_scalar_prefetch=1,
            grid=(DP, TOKENS // BI),
            in_specs=[
                whole((TOKENS, D)),
                whole((D, TOKENS)),
                whole((TOKENS, D)),
                whole((D, TOKENS)),
                pl.BlockSpec((1, D, TILE), lambda r, i, me: (layer, 0, piece(r, me))),
                pl.BlockSpec((1, D, TILE), lambda r, i, me: (layer, 0, piece(r, me))),
                pl.BlockSpec((1, TILE, D), lambda r, i, me: (layer, piece(r, me), 0)),
            ],
            out_specs=out_specs,
            scratch_shapes=[pltpu.VMEM((D, TILE), F32)] * 3 + [pltpu.VMEM((BI, TILE), BF16)] * 3,
        ),
        out_shape=outs,
        compiler_params=params(2),
        cost_estimate=cost((8 if with_da else 6) / CHUNKS, 30e6),
    )(me, a, at, dy, dyt, wg, wu, wd)


CI = 512


def between_kernel(h_ref, dy_ref, *refs):
    *parts, out_ref, outt_ref = refs
    da = parts[0][...]
    for part in parts[1:]:
        da = da + part[...]
    da = da.astype(BF16).astype(F32)
    wide = h_ref[...].astype(F32)
    scale = lax.rsqrt(jnp.mean(wide * wide, -1, keepdims=True) + 1e-6)
    dot_h = jnp.mean(da * wide, -1, keepdims=True)
    dh = (da * scale - wide * (scale * scale * scale * dot_h)).astype(BF16)
    dh = dy_ref[...] + dh
    out_ref[...] = dh
    outt_ref[...] = flipped(dh)


def between(h, dy, parts):
    block = pl.BlockSpec((CI, D), lambda i: (i, 0))
    return pl.pallas_call(
        between_kernel,
        grid=(TOKENS // CI,),
        in_specs=[block] * (2 + len(parts)),
        out_specs=[block, pl.BlockSpec((D, CI), lambda i: (0, i))],
        out_shape=[jax.ShapeDtypeStruct((TOKENS, D), BF16), jax.ShapeDtypeStruct((D, TOKENS), BF16)],
        compiler_params=params(1),
        cost_estimate=cost(0.4, 26e6),
        name="between",
    )(h, dy, *parts)


def adamw_kernel(me_ref, f_ref, ggu, gd, wg, wu, wd, mg, mu, md, vg, vu, vd, *refs):
    ngu, nd, *mv = refs[-8:]
    factor = f_ref[0, 0]
    for k, (g, w, m, v, to) in enumerate(
        (
            (ggu.at[0], wg.at[0], mg.at[0], vg.at[0], ngu.at[0]),
            (ggu.at[1], wu.at[0], mu.at[0], vu.at[0], ngu.at[1]),
            (gd, wd.at[0], md.at[0], vd.at[0], nd),
        )
    ):
        g = g[...].astype(F32) * factor
        m = 0.9 * m[...] + 0.1 * g
        v = 0.95 * v[...] + 0.05 * g * g
        w = w[...].astype(F32)
        to[...] = (w - 0.02 * (m * lax.rsqrt(v + 1e-8) + 0.1 * w)).astype(BF16)
        mv[k][0] = m
        mv[3 + k][0] = v


def adamw(layer, chunk, me, factor, ggu, gd, weights, m, v, so_far):
    step = TILE // DP
    w_spec = pl.BlockSpec((1, ROWS, TILE), lambda o, me: (layer, me[0], o * CHUNKS + chunk))
    wd_spec = pl.BlockSpec((1, step, D), lambda o, me: (layer, (me[0] * CHUNKS + chunk) * DP + o, 0))
    mv_spec = pl.BlockSpec((1, ROWS, TILE), lambda o, me: (layer, 0, o * CHUNKS + chunk))
    mvd_spec = pl.BlockSpec((1, step, D), lambda o, me: (layer, chunk * DP + o, 0))
    gu_spec = pl.BlockSpec((2, ROWS, TILE), lambda o, me: (0, 0, o))
    d_spec = pl.BlockSpec((step, D), lambda o, me: (o, 0))
    mv_specs = [mv_spec, mv_spec, mvd_spec] * 2
    return pl.pallas_call(
        adamw_kernel,
        grid_spec=pltpu.PrefetchScalarGridSpec(
            num_scalar_prefetch=1,
            grid=(DP,),
            in_specs=[pl.BlockSpec(memory_space=pltpu.SMEM), gu_spec, d_spec, w_spec, w_spec, wd_spec, *mv_specs]
            + [pl.BlockSpec(memory_space=pl.ANY)] * len(so_far),
            out_specs=[gu_spec, d_spec, *mv_specs],
        ),
        out_shape=[jax.ShapeDtypeStruct((2, ROWS, OWN), BF16), jax.ShapeDtypeStruct((TILE, D), BF16)]
        + [jax.ShapeDtypeStruct(t.shape, F32) for t in (*m, *v)],
        input_output_aliases={13 + n: 2 + n for n in range(len(so_far))},
        compiler_params=params(1),
        cost_estimate=cost(0.25, 17e6),
        name="adamw",
    )(me, factor, ggu, gd, *weights, *m, *v, *so_far)


def assemble_kernel(me_ref, gu0, d0, gu1, d1, *refs):
    wg, wu, wd = refs[-3:]
    for q, (gu, d) in enumerate(((gu0, d0), (gu1, d1))):

        @pl.when(pl.program_id(0) == q)
        def _(gu=gu, d=d):
            wg[0] = gu[0]
            wu[0] = gu[1]
            wd[0] = d[...]


def assemble(layer, chunk, base, me, first, second, so_far):
    step = TILE // DP

    def when(q, r, o):
        return jnp.where(r == q, o, 0 if q else DP - 1)

    def gu_spec(q):
        return pl.BlockSpec((2, ROWS, TILE), lambda r, o, me: (0, 0, when(q, r, o)))

    def d_spec(q):
        return pl.BlockSpec((step, D), lambda r, o, me: (when(q, r, o), 0))

    def owner(r, me):
        return (r + base) ^ me[0]

    w_spec = pl.BlockSpec((1, ROWS, TILE), lambda r, o, me: (layer, owner(r, me), o * CHUNKS + chunk))
    wd_spec = pl.BlockSpec((1, step, D), lambda r, o, me: (layer, (owner(r, me) * CHUNKS + chunk) * DP + o, 0))
    wide, tall = jax.ShapeDtypeStruct((LAYERS, D, FF), BF16), jax.ShapeDtypeStruct((LAYERS, FF, D), BF16)
    return pl.pallas_call(
        assemble_kernel,
        grid_spec=pltpu.PrefetchScalarGridSpec(
            num_scalar_prefetch=1,
            grid=(2, DP),
            in_specs=[gu_spec(0), d_spec(0), gu_spec(1), d_spec(1)] + [pl.BlockSpec(memory_space=pl.ANY)] * len(so_far),
            out_specs=[w_spec, w_spec, wd_spec],
        ),
        out_shape=[wide, wide, tall],
        input_output_aliases={5 + n: n for n in range(len(so_far))},
        compiler_params=params(2),
        cost_estimate=cost(0.15, 6e6),
        name="assemble",
    )(me, *first, *second, *so_far)


def to_core(t):
    return lax.ppermute(t, "dp", [(0, 1), (1, 0), (2, 3), (3, 2)])


def to_x(t):
    return lax.ppermute(t, "dp", [(0, 2), (2, 0), (1, 3), (3, 1)])


def solution(mesh):
    def body(x, dy, *arrays):
        weights, m, v = (arrays[i : i + 3] for i in (0, 3, 6))
        x, dy = x[0], dy[0]
        me = lax.axis_index("dp").astype(jnp.int32)[None]

        h1, a0, a1, a0t, a1t, dyt = forward(x, dy, *weights)

        gradients, given, summed = {}, {}, {}
        order = [(layer, chunk) for layer in (1, 0) for chunk in range(CHUNKS)]

        def give(k):
            _, _, give_gu, _, _, give_d = parts[k]
            given[k] = to_core(give_gu), to_core(give_d)

        def exchange(k):
            _, far_gu, _, _, far_d, _ = parts[k]
            got_gu, got_d = given[k]
            sum_gu = (far_gu.astype(F32) + got_gu[1].astype(F32)).astype(BF16)
            sum_d = (far_d.astype(F32) + got_d[1].astype(F32)).astype(BF16)
            summed[k] = to_x(sum_gu), to_x(sum_d)

        def finish(k):
            own_gu, _, _, own_d, _, _ = parts[k]
            (got_gu, got_d), (sum_gu, sum_d) = given[k], summed[k]
            gu = (own_gu.astype(F32) + got_gu[0].astype(F32) + sum_gu.astype(F32)).astype(BF16)
            d = (own_d.astype(F32) + got_d[0].astype(F32) + sum_d.astype(F32)).astype(BF16)
            squares = jnp.sum(jnp.square(gu.astype(F32))) + jnp.sum(jnp.square(d.astype(F32)))
            gradients[order[k]] = gu, d, squares

        da, parts = [], {}
        for k, (layer, chunk) in enumerate(order):
            if k == CHUNKS:
                dh, dht = between(h1, dy, da)
            if layer:
                *parts[k], part = backward(1, chunk, True, me, a1, a1t, dy, dyt, *weights)
                da.append(part)
            else:
                parts[k] = backward(0, chunk, False, me, a0, a0t, dh, dht, *weights)
            give(k)
            exchange(k)
        for k in range(8):
            finish(k)

        total = lax.psum(sum(g[2] for g in gradients.values()), "dp")
        factor = jnp.minimum(1.0, 0.5 * lax.rsqrt(total / COUNT + 1e-30)).reshape(1, 1)

        moments, new, own = (), (), {}
        for k, ((layer, chunk), (gu, d, _)) in enumerate(gradients.items()):
            own_gu, own_d, *moments = adamw(layer, chunk, me, factor, gu, d, weights, m, v, moments)
            own[k] = own_gu, own_d
        for k, (layer, chunk) in enumerate(gradients):
            far = tuple(map(to_x, own[k]))
            near = tuple(map(to_core, own[k]))
            last = tuple(map(to_core, far))
            new = assemble(layer, chunk, 0, me, own[k], near, new)
            new = assemble(layer, chunk, 2, me, far, last, new)
        return (*new, *moments)

    rows = P(None, "dp", None)
    return jax.shard_map(
        body,
        mesh=mesh,
        in_specs=(P(("rep", "dp"), None, None),) * 2 + (P(None, None, None),) * 3 + (rows,) * 6,
        out_specs=(P("rep", None, None),) * 3 + (P("rep", "dp", None),) * 6,
        check_vma=False,
    )
```

```python
import jax
import jax.numpy as jnp
from jax import lax
from jax.experimental import pallas as pl
from jax.experimental.pallas import tpu as pltpu
from jax.sharding import PartitionSpec as P


F32, BF16 = jnp.float32, jnp.bfloat16
TOKENS, D, FF = 2048, 512, 8192
LAYERS, DP = 2, 4
OWN = FF // DP
SIZE = 256
PARTS = OWN // SIZE
STEPS = LAYERS * PARTS * DP
SLOTS = 3
CHUNKS = [(1, start, 512) for start in range(0, OWN, 512)] + [(0, 0, 512), (0, 512, 512), (0, 1024, 512), (0, 1536, 256), (0, 1792, 256)]
LAST = len(CHUNKS) - 1
ROWS = D // DP
COUNT = 3 * LAYERS * D * FF
VMEM = 60 * 1024 * 1024


def dot(a, b):
    return jnp.dot(a, b, preferred_element_type=F32)


def dot_nt(a, b):
    return lax.dot_general(a, b, (((1,), (1,)), ((), ())), preferred_element_type=F32)


def sigmoid(x):
    return 0.5 * jnp.tanh(0.5 * x) + 0.5


def normed(h):
    wide = h.astype(F32)
    return (wide * lax.rsqrt(jnp.mean(wide * wide, -1, keepdims=True) + 1e-6)).astype(BF16)


def flipped(t):
    return t.astype(F32).T.astype(BF16)


def whole(shape):
    return pl.BlockSpec(shape, lambda *_: (0,) * len(shape), pipeline_mode=pl.Buffered(1))


def params(n):
    return pltpu.CompilerParams(dimension_semantics=("arbitrary",) * n, vmem_limit_bytes=VMEM)


def cost(units, moved):
    return pl.CostEstimate(flops=int(units * 2 * TOKENS * D * FF), bytes_accessed=int(moved), transcendentals=0)


FT, FI = 1024, 2048


def forward_kernel(x_ref, dy_ref, wg_ref, wu_ref, wd_ref, h1_ref, a0_ref, a1_ref, a0t_ref, a1t_ref, dyt_ref, acc_ref, z_ref):
    j, i = pl.program_id(0), pl.program_id(1)
    rows = pl.ds(pl.multiple_of(i * FI, FI), FI)

    @pl.when(j == 0)
    def _():
        a = normed(x_ref[rows, :])
        a0_ref[rows, :] = a
        a0t_ref[:, rows] = flipped(a)
        dyt_ref[:, rows] = flipped(dy_ref[rows, :])
        acc_ref[rows, :] = jnp.zeros((FI, D), F32)

    a = a0_ref[rows, :]
    for s in range(0, FT, 256):
        gate = dot(a, wg_ref[0, :, s : s + 256])
        up = dot(a, wu_ref[0, :, s : s + 256])
        z_ref[:, s : s + 256] = (gate * sigmoid(gate) * up).astype(BF16)
    acc_ref[rows, :] += dot(z_ref[...], wd_ref[0])

    @pl.when(j == FF // FT - 1)
    def _():
        h1 = x_ref[rows, :] + acc_ref[rows, :].astype(BF16)
        a1 = normed(h1)
        h1_ref[rows, :] = h1
        a1_ref[rows, :] = a1
        a1t_ref[:, rows] = flipped(a1)


def forward(x, dy, wg, wu, wd):
    row, col = jax.ShapeDtypeStruct((TOKENS, D), BF16), jax.ShapeDtypeStruct((D, TOKENS), BF16)
    return pl.pallas_call(
        forward_kernel,
        grid=(FF // FT, TOKENS // FI),
        in_specs=[
            whole((TOKENS, D)),
            whole((TOKENS, D)),
            pl.BlockSpec((1, D, FT), lambda j, i: (0, 0, j)),
            pl.BlockSpec((1, D, FT), lambda j, i: (0, 0, j)),
            pl.BlockSpec((1, FT, D), lambda j, i: (0, j, 0)),
        ],
        out_specs=[whole((TOKENS, D))] * 3 + [whole((D, TOKENS))] * 3,
        out_shape=[row] * 3 + [col] * 3,
        scratch_shapes=[pltpu.VMEM((TOKENS, D), F32), pltpu.VMEM((FI, FT), BF16)],
        compiler_params=params(2),
        cost_estimate=cost(3, 40e6),
        name="forward0",
    )(x, dy, wg, wu, wd)


BI = 512


def backward_kernel(
    h1, a0, a0t, a1, a1t, dy0, dy0t, wg, wu, wd, gu_out, d_out, squares,
    a, at, dy, dyt, h, da, wgu_buf, wd_buf, z, dgu, dt, grads,
    own_gu, far_gu, give_gu, core_gu, x_gu, own_d, far_d, give_d, core_d, x_d,
    w_sem, in_sem, core_send, core_recv, x_send, x_recv, out_sem, core_free, x_free,
):
    t = pl.program_id(0)
    part, r = lax.div(t, DP), lax.rem(t, DP)
    slot = lax.rem(part, SLOTS)
    rep, me = lax.axis_index("rep"), lax.axis_index("dp")
    mx, mc = lax.div(me, 2), lax.rem(me, 2)

    def related(qx, qc):
        return lax.rem(mx + qx, 2) * 2 + lax.rem(mc + qc, 2)

    core_peer, x_peer = (rep, related(0, 1)), (rep, related(1, 0))
    mesh_id = pl.DeviceIdType.MESH

    def weights(t):
        part, r = lax.div(t, DP), lax.rem(t, DP)
        layer = 1 - lax.div(part, PARTS)
        at_ff = pl.multiple_of(related(lax.div(r, 2), lax.rem(r, 2)) * OWN + lax.rem(part, PARTS) * SIZE, SIZE)
        n = lax.rem(t, 2)
        return (
            pltpu.make_async_copy(wg.at[layer, :, pl.ds(at_ff, SIZE)], wgu_buf.at[n, :, 0:SIZE], w_sem.at[n, 0]),
            pltpu.make_async_copy(wu.at[layer, :, pl.ds(at_ff, SIZE)], wgu_buf.at[n, :, SIZE : 2 * SIZE], w_sem.at[n, 1]),
            pltpu.make_async_copy(wd.at[layer, pl.ds(at_ff, SIZE), :], wd_buf.at[n], w_sem.at[n, 2]),
        )

    def inputs(*sources):
        pairs = zip(sources, (a, at, dy, dyt, h))
        return [pltpu.make_async_copy(src, dst, in_sem.at[n]) for n, (src, dst) in enumerate(pairs)]

    def to_core(n):
        return [
            pltpu.make_async_remote_copy(src.at[n], dst.at[n], core_send.at[n, i], core_recv.at[n, i], device_id=core_peer, device_id_type=mesh_id)
            for i, (src, dst) in enumerate(((give_gu, core_gu), (give_d, core_d)))
        ]

    def to_x(n):
        return [
            pltpu.make_async_remote_copy(src.at[n], dst.at[n], x_send.at[n, i], x_recv.at[n, i], device_id=x_peer, device_id_type=mesh_id)
            for i, (src, dst) in enumerate(((far_gu, x_gu), (far_d, x_d)))
        ]

    def out(p, n):
        return [
            pltpu.make_async_copy(src.at[n], dst.at[p], out_sem.at[n, i]) for i, (src, dst) in enumerate(((own_gu, gu_out), (own_d, d_out)))
        ]

    def give(p):
        n = lax.rem(p, SLOTS)

        @pl.when(p >= SLOTS)
        def _():
            pl.semaphore_wait(core_free, 1)

        for copy in to_core(n):
            copy.start()

    def pair(p):
        n = lax.rem(p, SLOTS)
        for copy in to_core(n):
            copy.wait_recv()
        far_gu[n] = (far_gu[n].astype(F32) + core_gu[n, 1].astype(F32)).astype(BF16)
        far_d[n] = (far_d[n].astype(F32) + core_d[n, 1].astype(F32)).astype(BF16)

        @pl.when(p >= SLOTS)
        def _():
            pl.semaphore_wait(x_free, 1)

        for copy in to_x(n):
            copy.start()

    def finish(p):
        n = lax.rem(p, SLOTS)
        for copy in to_x(n):
            copy.wait()
        for copy in to_core(n):
            copy.wait_send()
        total = (own_gu[n].astype(F32) + core_gu[n, 0].astype(F32) + x_gu[n].astype(F32)).astype(BF16)
        own_gu[n] = total
        total = total.astype(F32)
        line = jnp.sum(total[0] * total[0] + total[1] * total[1], 0, keepdims=True)
        line = sum(line[:, i : i + D] for i in range(0, line.shape[1], D))
        total = (own_d[n].astype(F32) + core_d[n, 0].astype(F32) + x_d[n].astype(F32)).astype(BF16)
        own_d[n] = total
        total = total.astype(F32)
        squares[...] += line + jnp.sum(total * total, 0, keepdims=True)

        @pl.when(p < LAYERS * PARTS - SLOTS)
        def _():
            pl.semaphore_signal(core_free, inc=1, device_id=core_peer, device_id_type=mesh_id)
            pl.semaphore_signal(x_free, inc=1, device_id=x_peer, device_id_type=mesh_id)

        for copy in out(p, n):
            copy.start()

    @pl.when(t == 0)
    def _():
        barrier = pltpu.get_barrier_semaphore()
        for peer in (core_peer, x_peer):
            pl.semaphore_signal(barrier, inc=1, device_id=peer, device_id_type=mesh_id)
        for copy in (*weights(t), *inputs(a1, a1t, dy0, dy0t, h1)):
            copy.start()
        da[...] = jnp.zeros_like(da)
        squares[...] = jnp.zeros_like(squares)
        for copy in inputs(a1, a1t, dy0, dy0t, h1):
            copy.wait()
        pl.semaphore_wait(barrier, 2)

    for copy in weights(t):
        copy.wait()

    @pl.when(t < STEPS - 1)
    def _():
        for copy in weights(t + 1):
            copy.start()

    @pl.when(t == STEPS // 2)
    def _():
        for copy in inputs(a0, a0t):
            copy.start()
        for b in range(0, TOKENS, BI):
            rows = slice(b, b + BI)
            back = da[rows, :].astype(BF16).astype(F32)
            wide = h[rows, :].astype(F32)
            scale = lax.rsqrt(jnp.mean(wide * wide, -1, keepdims=True) + 1e-6)
            along = jnp.mean(back * wide, -1, keepdims=True)
            dh = dy[rows, :] + (back * scale - wide * (scale * scale * scale * along)).astype(BF16)
            dy[rows, :] = dh
            dyt[:, rows] = flipped(dh)
        for copy in inputs(a0, a0t):
            copy.wait()

    def tile(with_da):
        w = lax.rem(t, 2)
        for b in range(0, TOKENS, BI):
            rows = slice(b, b + BI)
            both = dot(a[rows, :], wgu_buf[w])
            gate, up = both[:, :SIZE], both[:, SIZE:]
            dz = dot_nt(dy[rows, :], wd_buf[w]).astype(BF16).astype(F32)
            sig = sigmoid(gate)
            act = gate * sig
            z[rows, :] = (act * up).astype(BF16)
            dgu[rows, SIZE : 2 * SIZE] = (dz * act).astype(BF16)
            dgu[rows, 0:SIZE] = (dz * up * (sig + act * (1.0 - sig))).astype(BF16)
        dt[...] = dot(dyt[...], z[...]).T.astype(BF16)
        grads[...] = dot(at[...], dgu[...]).astype(BF16)
        if with_da:
            for b in range(0, TOKENS, BI):
                rows = slice(b, b + BI)
                da[rows, :] += dot_nt(dgu[rows, :], wgu_buf[w])

    @pl.when(t < STEPS // 2)
    def _():
        tile(True)

    @pl.when(t >= STEPS // 2)
    def _():
        tile(False)

    columns = pl.ds(pl.multiple_of(related(lax.div(r, 2), lax.rem(r, 2)) * SIZE, SIZE), SIZE)
    for q, (gu, d) in enumerate(((own_gu, own_d), (give_gu.at[:, 0], give_d.at[:, 0]), (far_gu, far_d), (give_gu.at[:, 1], give_d.at[:, 1]))):
        rows = pl.ds(pl.multiple_of(related(q // 2, q % 2) * ROWS, ROWS), ROWS)
        for i in range(2):
            gu[slot, i, :, columns] = grads[rows, i * SIZE : (i + 1) * SIZE]

        @pl.when(r == q)
        def _(d=d):
            d[slot] = dt[...]

    @pl.when((r == 0) & (part >= 1))
    def _():
        pair(part - 1)

    @pl.when((r == 2) & (part >= 2))
    def _():
        finish(part - 2)

    @pl.when((r == 3) & (part >= 2))
    def _():
        for copy in out(part - 2, lax.rem(part - 2, SLOTS)):
            copy.wait()

    @pl.when(r == 3)
    def _():
        give(part)

    @pl.when(t == STEPS - 1)
    def _():
        pair(part)
        finish(part - 1)
        finish(part)
        for p in (part - 1, part):
            for copy in out(p, lax.rem(p, SLOTS)):
                copy.wait()


def backward(h1, a0, a0t, a1, a1t, dy, dyt, wg, wu, wd):
    wide = DP * SIZE
    row, col, vm, dma = (TOKENS, D), (D, TOKENS), pltpu.VMEM, pltpu.SemaphoreType.DMA
    gu, d = (SLOTS, 2, ROWS, wide), (SLOTS, SIZE, D)
    two_gu, two_d = (SLOTS, 2, 2, ROWS, wide), (SLOTS, 2, SIZE, D)
    return pl.pallas_call(
        backward_kernel,
        grid=(STEPS,),
        in_specs=[pl.BlockSpec(memory_space=pl.ANY)] * 10,
        out_specs=[pl.BlockSpec(memory_space=pl.ANY)] * 2 + [pl.BlockSpec((1, D), lambda t: (0, 0))],
        out_shape=[
            jax.ShapeDtypeStruct((LAYERS * PARTS, 2, ROWS, wide), BF16),
            jax.ShapeDtypeStruct((LAYERS * PARTS, SIZE, D), BF16),
            jax.ShapeDtypeStruct((1, D), F32),
        ],
        scratch_shapes=[
            *(vm(shape, BF16) for shape in (row, col, row, col, row)),
            vm(row, F32),
            *(vm(shape, BF16) for shape in ((2, D, 2 * SIZE), (2, SIZE, D), (TOKENS, SIZE), (TOKENS, 2 * SIZE), (SIZE, D), (D, 2 * SIZE))),
            *(vm(shape, BF16) for shape in (gu, gu, two_gu, two_gu, gu, d, d, two_d, two_d, d)),
            dma((2, 3)),
            dma((5,)),
            *[dma((SLOTS, 2))] * 5,
            pltpu.SemaphoreType.REGULAR,
            pltpu.SemaphoreType.REGULAR,
        ],
        compiler_params=pltpu.CompilerParams(
            dimension_semantics=("arbitrary",), vmem_limit_bytes=VMEM, collective_id=0, has_side_effects=True
        ),
        cost_estimate=cost(14, 120e6),
        name="backward",
    )(h1, a0, a0t, a1, a1t, dy, dyt, wg, wu, wd)


def adamw_kernel(me_ref, f_ref, ggu, gd, wg, wu, wd, mg, mu, md, vg, vu, vd, *refs):
    ngu, nd, *mv = refs[-8:]
    factor = f_ref[0, 0]
    for k, (g, w, m, v, to) in enumerate(
        (
            (jnp.concatenate([ggu[p, 0] for p in range(ggu.shape[0])], 1), wg.at[0], mg.at[0], vg.at[0], ngu.at[0]),
            (jnp.concatenate([ggu[p, 1] for p in range(ggu.shape[0])], 1), wu.at[0], mu.at[0], vu.at[0], ngu.at[1]),
            (gd[...], wd.at[0], md.at[0], vd.at[0], nd),
        )
    ):
        g = g.astype(F32) * factor
        m = 0.9 * m[...] + 0.1 * g
        v = 0.95 * v[...] + 0.05 * g * g
        w = w[...].astype(F32)
        to[...] = (w - 0.02 * (m * lax.rsqrt(v + 1e-8) + 0.1 * w)).astype(BF16)
        mv[k][0] = m
        mv[3 + k][0] = v


def adamw(chunk, me, factor, ggu, gd, weights, m, v, so_far):
    layer, start, size = chunk
    step = size // DP
    w_spec = pl.BlockSpec((1, ROWS, size), lambda o, me: (layer, me[0], (o * OWN + start) // size))
    wd_spec = pl.BlockSpec((1, step, D), lambda o, me: (layer, (me[0] * OWN + start) // step + o, 0))
    mv_spec = pl.BlockSpec((1, ROWS, size), lambda o, me: (layer, 0, (o * OWN + start) // size))
    mvd_spec = pl.BlockSpec((1, step, D), lambda o, me: (layer, start // step + o, 0))
    gu_spec = pl.BlockSpec((2, ROWS, size), lambda o, me: (0, 0, o))
    d_spec = pl.BlockSpec((step, D), lambda o, me: (o, 0))
    part, parts = (1 - layer) * PARTS + start // SIZE, size // SIZE
    ggu_spec = pl.BlockSpec((parts, 2, ROWS, SIZE), lambda o, me: (part // parts, 0, 0, o))
    gd_spec = pl.BlockSpec((step, D), lambda o, me: (part * SIZE // step + o, 0))
    mv_specs = [mv_spec, mv_spec, mvd_spec] * 2
    return pl.pallas_call(
        adamw_kernel,
        grid_spec=pltpu.PrefetchScalarGridSpec(
            num_scalar_prefetch=1,
            grid=(DP,),
            in_specs=[pl.BlockSpec(memory_space=pltpu.SMEM), ggu_spec, gd_spec, w_spec, w_spec, wd_spec, *mv_specs]
            + [pl.BlockSpec(memory_space=pl.ANY)] * len(so_far),
            out_specs=[gu_spec, d_spec, *mv_specs],
        ),
        out_shape=[jax.ShapeDtypeStruct((2, ROWS, DP * size), BF16), jax.ShapeDtypeStruct((size, D), BF16)]
        + [jax.ShapeDtypeStruct(t.shape, F32) for t in (*m, *v)],
        input_output_aliases={13 + n: 2 + n for n in range(len(so_far))},
        compiler_params=params(1),
        cost_estimate=cost(0.25, 17e6),
        name="adamw",
    )(me, factor, ggu, gd, *weights, *m, *v, *so_far)


def assemble_kernel(me_ref, gu0, d0, gu1, d1, *refs):
    wg, wu, wd = refs[-3:]
    for q, (gu, d) in enumerate(((gu0, d0), (gu1, d1))):

        @pl.when(pl.program_id(0) == q)
        def _(gu=gu, d=d):
            wg[0] = gu[0]
            wu[0] = gu[1]
            wd[0] = d[...]


def assemble(chunk, base, me, first, second, so_far):
    layer, start, size = chunk
    step = size // DP

    def when(q, r, o):
        return jnp.where(r == q, o, 0 if q else DP - 1)

    def gu_spec(q):
        return pl.BlockSpec((2, ROWS, size), lambda r, o, me: (0, 0, when(q, r, o)))

    def d_spec(q):
        return pl.BlockSpec((step, D), lambda r, o, me: (when(q, r, o), 0))

    def owner(r, me):
        return (r + base) ^ me[0]

    w_spec = pl.BlockSpec((1, ROWS, size), lambda r, o, me: (layer, owner(r, me), (o * OWN + start) // size))
    wd_spec = pl.BlockSpec((1, step, D), lambda r, o, me: (layer, (owner(r, me) * OWN + start) // step + o, 0))
    wide, tall = jax.ShapeDtypeStruct((LAYERS, D, FF), BF16), jax.ShapeDtypeStruct((LAYERS, FF, D), BF16)
    return pl.pallas_call(
        assemble_kernel,
        grid_spec=pltpu.PrefetchScalarGridSpec(
            num_scalar_prefetch=1,
            grid=(2, DP),
            in_specs=[gu_spec(0), d_spec(0), gu_spec(1), d_spec(1)] + [pl.BlockSpec(memory_space=pl.ANY)] * len(so_far),
            out_specs=[w_spec, w_spec, wd_spec],
        ),
        out_shape=[wide, wide, tall],
        input_output_aliases={5 + n: n for n in range(len(so_far))},
        compiler_params=params(2),
        cost_estimate=cost(0.15, 6e6),
        name="assemble",
    )(me, *first, *second, *so_far)


def to_core(t):
    return lax.ppermute(t, "dp", [(0, 1), (1, 0), (2, 3), (3, 2)])


def to_x(t):
    return lax.ppermute(t, "dp", [(0, 2), (2, 0), (1, 3), (3, 1)])


def solution(mesh):
    def body(x, dy, *arrays):
        weights, m, v = (arrays[i : i + 3] for i in (0, 3, 6))
        x, dy = x[0], dy[0]
        me = lax.axis_index("dp").astype(jnp.int32)[None]

        h1, a0, a1, a0t, a1t, dyt = forward(x, dy, *weights)

        gu, d, squares = backward(h1, a0, a0t, a1, a1t, dy, dyt, *weights)
        d = d.reshape(-1, D)
        total = lax.psum(jnp.sum(squares), "dp")
        factor = jnp.minimum(1.0, 0.5 * lax.rsqrt(total / COUNT + 1e-30)).reshape(1, 1)

        moments, own, near, far, last, new = (), {}, {}, {}, {}, ()
        turn = [LAST - 1, *range(LAST - 1), LAST]
        for n, k in enumerate(turn):
            own_gu, own_d, *moments = adamw(CHUNKS[k], me, factor, gu, d, weights, m, v, moments)
            own[n] = own_gu, own_d
            far[n] = tuple(map(to_x, own[n]))
            near[n] = tuple(map(to_core, own[n]))
            last[n] = tuple(map(to_core, far[n]))
        for n in range(LAST + 1):
            for ahead in (0, 1, 2) if n == 0 else (n + 2,):
                if ahead <= LAST:
                    new = assemble(CHUNKS[turn[ahead]], 0, me, own[ahead], near[ahead], new)
            new = assemble(CHUNKS[turn[n]], 2, me, far[n], last[n], new)
        return (*new, *moments)

    rows = P(None, "dp", None)
    return jax.shard_map(
        body,
        mesh=mesh,
        in_specs=(P(("rep", "dp"), None, None),) * 2 + (P(None, None, None),) * 3 + (rows,) * 6,
        out_specs=(P("rep", None, None),) * 3 + (P("rep", "dp", None),) * 6,
        check_vma=False,
    )
```

```python
import functools

import jax
import jax.numpy as jnp
from jax import lax
from jax.experimental import pallas as pl
from jax.experimental.pallas import tpu as pltpu
from jax.sharding import PartitionSpec as P


F32, BF16 = jnp.float32, jnp.bfloat16
TOKENS, D, FF = 2048, 512, 8192
LAYERS, DP = 2, 4
OWN = FF // DP
SIZE = 256
PARTS = OWN // SIZE
STEPS = LAYERS * PARTS * DP
SLOTS = 3
CHUNKS = [(1, start, 512) for start in range(0, OWN, 512)] + [(0, 0, 512), (0, 512, 512), (0, 1024, 512), (0, 1536, 256), (0, 1792, 256)]
LAST = len(CHUNKS) - 1
ROWS = D // DP
COUNT = 3 * LAYERS * D * FF
VMEM = 60 * 1024 * 1024


def dot(a, b):
    return jnp.dot(a, b, preferred_element_type=F32)


def dot_nt(a, b):
    return lax.dot_general(a, b, (((1,), (1,)), ((), ())), preferred_element_type=F32)


def sigmoid(x):
    return 0.5 * jnp.tanh(0.5 * x) + 0.5


def normed(h):
    wide = h.astype(F32)
    return (wide * lax.rsqrt(jnp.mean(wide * wide, -1, keepdims=True) + 1e-6)).astype(BF16)


def flipped(t):
    return t.astype(F32).T.astype(BF16)


def whole(shape):
    return pl.BlockSpec(shape, lambda *_: (0,) * len(shape), pipeline_mode=pl.Buffered(1))


def params(n):
    return pltpu.CompilerParams(dimension_semantics=("arbitrary",) * n, vmem_limit_bytes=VMEM)


def cost(units, moved):
    return pl.CostEstimate(flops=int(units * 2 * TOKENS * D * FF), bytes_accessed=int(moved), transcendentals=0)


FT, FI = 1024, 2048


def forward_kernel(x_ref, dy_ref, wg_ref, wu_ref, wd_ref, h1_ref, a0_ref, a1_ref, a0t_ref, a1t_ref, dyt_ref, acc_ref, z_ref):
    j, i = pl.program_id(0), pl.program_id(1)
    rows = pl.ds(pl.multiple_of(i * FI, FI), FI)

    @pl.when(j == 0)
    def _():
        a = normed(x_ref[rows, :])
        a0_ref[rows, :] = a
        a0t_ref[:, rows] = flipped(a)
        dyt_ref[:, rows] = flipped(dy_ref[rows, :])
        acc_ref[rows, :] = jnp.zeros((FI, D), F32)

    a = a0_ref[rows, :]
    for s in range(0, FT, 256):
        gate = dot(a, wg_ref[0, :, s : s + 256])
        up = dot(a, wu_ref[0, :, s : s + 256])
        z_ref[:, s : s + 256] = (gate * sigmoid(gate) * up).astype(BF16)
    acc_ref[rows, :] += dot(z_ref[...], wd_ref[0])

    @pl.when(j == FF // FT - 1)
    def _():
        h1 = x_ref[rows, :] + acc_ref[rows, :].astype(BF16)
        a1 = normed(h1)
        h1_ref[rows, :] = h1
        a1_ref[rows, :] = a1
        a1t_ref[:, rows] = flipped(a1)


def forward(x, dy, wg, wu, wd):
    row, col = jax.ShapeDtypeStruct((TOKENS, D), BF16), jax.ShapeDtypeStruct((D, TOKENS), BF16)
    return pl.pallas_call(
        forward_kernel,
        grid=(FF // FT, TOKENS // FI),
        in_specs=[
            whole((TOKENS, D)),
            whole((TOKENS, D)),
            pl.BlockSpec((1, D, FT), lambda j, i: (0, 0, j)),
            pl.BlockSpec((1, D, FT), lambda j, i: (0, 0, j)),
            pl.BlockSpec((1, FT, D), lambda j, i: (0, j, 0)),
        ],
        out_specs=[whole((TOKENS, D))] * 3 + [whole((D, TOKENS))] * 3,
        out_shape=[row] * 3 + [col] * 3,
        scratch_shapes=[pltpu.VMEM((TOKENS, D), F32), pltpu.VMEM((FI, FT), BF16)],
        compiler_params=params(2),
        cost_estimate=cost(3, 40e6),
        name="forward0",
    )(x, dy, wg, wu, wd)


BI = 512


def backward_kernel(
    h1, a0, a0t, a1, a1t, dy0, dy0t, wg, wu, wd, gu_out, d_out, squares,
    a, at, dy, dyt, h, da, wgu_buf, wd_buf, z, dgu, dt, grads,
    own_gu, far_gu, give_gu, core_gu, x_gu, own_d, far_d, give_d, core_d, x_d, sq,
    w_sem, in_sem, core_send, core_recv, x_send, x_recv, out_sem, sq_send, sq_recv, core_free, x_free,
):
    t = pl.program_id(0)
    part, turn = lax.div(t, DP), lax.rem(t, DP)
    r = lax.rem(turn + 2, DP)
    slot = lax.rem(part, SLOTS)
    rep, me = lax.axis_index("rep"), lax.axis_index("dp")
    mx, mc = lax.div(me, 2), lax.rem(me, 2)

    def related(qx, qc):
        return lax.rem(mx + qx, 2) * 2 + lax.rem(mc + qc, 2)

    core_peer, x_peer = (rep, related(0, 1)), (rep, related(1, 0))
    mesh_id = pl.DeviceIdType.MESH

    def weights(t):
        part, r = lax.div(t, DP), lax.rem(t + 2, DP)
        layer = 1 - lax.div(part, PARTS)
        at_ff = pl.multiple_of(related(lax.div(r, 2), lax.rem(r, 2)) * OWN + lax.rem(part, PARTS) * SIZE, SIZE)
        n = lax.rem(t, 2)
        return (
            pltpu.make_async_copy(wg.at[layer, :, pl.ds(at_ff, SIZE)], wgu_buf.at[n, :, 0:SIZE], w_sem.at[n, 0]),
            pltpu.make_async_copy(wu.at[layer, :, pl.ds(at_ff, SIZE)], wgu_buf.at[n, :, SIZE : 2 * SIZE], w_sem.at[n, 1]),
            pltpu.make_async_copy(wd.at[layer, pl.ds(at_ff, SIZE), :], wd_buf.at[n], w_sem.at[n, 2]),
        )

    def inputs(*sources):
        pairs = zip(sources, (a, at, dy, dyt, h))
        return [pltpu.make_async_copy(src, dst, in_sem.at[n]) for n, (src, dst) in enumerate(pairs)]

    def columns_of(half):
        return pl.ds(pl.multiple_of((mx if half else 1 - mx) * 2 * SIZE, 2 * SIZE), 2 * SIZE)

    def remote(src, dst, send, recv, peer):
        return pltpu.make_async_remote_copy(src, dst, send, recv, device_id=peer, device_id_type=mesh_id)

    def to_core(n, half):
        c = columns_of(half)
        pairs = ((give_gu.at[n, :, :, :, c], core_gu.at[n, :, :, :, c]), (give_d.at[n, 1 - half], core_d.at[n, 1 - half]))
        return [remote(src, dst, core_send.at[n, half, i], core_recv.at[n, half, i], core_peer) for i, (src, dst) in enumerate(pairs)]

    def to_x(n, half):
        c = columns_of(half)
        pairs = ((far_gu.at[n, :, :, c], x_gu.at[n, :, :, c]), (far_d.at[n], x_d.at[n]))[: 2 - half]
        return [remote(src, dst, x_send.at[n, half, i], x_recv.at[n, half, i], x_peer) for i, (src, dst) in enumerate(pairs)]

    def out(p, n):
        return [
            pltpu.make_async_copy(src.at[n], dst.at[p], out_sem.at[n, i]) for i, (src, dst) in enumerate(((own_gu, gu_out), (own_d, d_out)))
        ]

    def give(p, half):
        n = lax.rem(p, SLOTS)
        if half == 0:

            @pl.when(p >= SLOTS)
            def _():
                pl.semaphore_wait(core_free, 1)

        for copy in to_core(n, half):
            copy.start()

    def pair(p, half):
        n = lax.rem(p, SLOTS)
        for copy in to_core(n, half):
            copy.wait_recv()
        c = columns_of(half)
        far_gu[n, :, :, c] = (far_gu[n, :, :, c].astype(F32) + core_gu[n, 1, :, :, c].astype(F32)).astype(BF16)
        if half == 0:
            far_d[n] = (far_d[n].astype(F32) + core_d[n, 1].astype(F32)).astype(BF16)

            @pl.when(p >= SLOTS)
            def _():
                pl.semaphore_wait(x_free, 1)

        for copy in to_x(n, half):
            copy.start()

    def finish(p):
        n = lax.rem(p, SLOTS)
        for half in range(2):
            for copy in to_x(n, half):
                copy.wait()
            for copy in to_core(n, half):
                copy.wait_send()
        total = (own_gu[n].astype(F32) + core_gu[n, 0].astype(F32) + x_gu[n].astype(F32)).astype(BF16)
        own_gu[n] = total
        total = total.astype(F32)
        line = jnp.sum(total[0] * total[0] + total[1] * total[1], 0, keepdims=True)
        line = sum(line[:, i : i + D] for i in range(0, line.shape[1], D))
        total = (own_d[n].astype(F32) + core_d[n, 0].astype(F32) + x_d[n].astype(F32)).astype(BF16)
        own_d[n] = total
        total = total.astype(F32)
        sq[0, 0:1, :] += line + jnp.sum(total * total, 0, keepdims=True)

        @pl.when(p < LAYERS * PARTS - SLOTS)
        def _():
            pl.semaphore_signal(core_free, inc=1, device_id=core_peer, device_id_type=mesh_id)
            pl.semaphore_signal(x_free, inc=1, device_id=x_peer, device_id_type=mesh_id)

        for copy in out(p, n):
            copy.start()

    @pl.when(t == 0)
    def _():
        barrier = pltpu.get_barrier_semaphore()
        for peer in (core_peer, x_peer):
            pl.semaphore_signal(barrier, inc=1, device_id=peer, device_id_type=mesh_id)
        for copy in (*weights(t), *inputs(a1, a1t, dy0, dy0t, h1)):
            copy.start()
        da[...] = jnp.zeros_like(da)
        sq[...] = jnp.zeros_like(sq)
        for copy in inputs(a1, a1t, dy0, dy0t, h1):
            copy.wait()
        pl.semaphore_wait(barrier, 2)

    for copy in weights(t):
        copy.wait()

    @pl.when(t < STEPS - 1)
    def _():
        for copy in weights(t + 1):
            copy.start()

    @pl.when(t == STEPS // 2)
    def _():
        for copy in inputs(a0, a0t):
            copy.start()
        for b in range(0, TOKENS, BI):
            rows = slice(b, b + BI)
            back = da[rows, :].astype(BF16).astype(F32)
            wide = h[rows, :].astype(F32)
            scale = lax.rsqrt(jnp.mean(wide * wide, -1, keepdims=True) + 1e-6)
            along = jnp.mean(back * wide, -1, keepdims=True)
            dh = dy[rows, :] + (back * scale - wide * (scale * scale * scale * along)).astype(BF16)
            dy[rows, :] = dh
            dyt[:, rows] = flipped(dh)
        for copy in inputs(a0, a0t):
            copy.wait()

    def tile(with_da):
        w = lax.rem(t, 2)
        for b in range(0, TOKENS, BI):
            rows = slice(b, b + BI)
            both = dot(a[rows, :], wgu_buf[w])
            gate, up = both[:, :SIZE], both[:, SIZE:]
            dz = dot_nt(dy[rows, :], wd_buf[w]).astype(BF16).astype(F32)
            sig = sigmoid(gate)
            act = gate * sig
            z[rows, :] = (act * up).astype(BF16)
            dgu[rows, SIZE : 2 * SIZE] = (dz * act).astype(BF16)
            dgu[rows, 0:SIZE] = (dz * up * (sig + act * (1.0 - sig))).astype(BF16)
        dt[...] = dot(dyt[...], z[...]).T.astype(BF16)
        grads[...] = dot(at[...], dgu[...]).astype(BF16)
        if with_da:
            for b in range(0, TOKENS, BI):
                rows = slice(b, b + BI)
                da[rows, :] += dot_nt(dgu[rows, :], wgu_buf[w])

    @pl.when(t < STEPS // 2)
    def _():
        tile(True)

    @pl.when(t >= STEPS // 2)
    def _():
        tile(False)

    columns = pl.ds(pl.multiple_of(related(lax.div(r, 2), lax.rem(r, 2)) * SIZE, SIZE), SIZE)
    for q, (gu, d) in enumerate(((own_gu, own_d), (give_gu.at[:, 0], give_d.at[:, 0]), (far_gu, far_d), (give_gu.at[:, 1], give_d.at[:, 1]))):
        rows = pl.ds(pl.multiple_of(related(q // 2, q % 2) * ROWS, ROWS), ROWS)
        for i in range(2):
            gu[slot, i, :, columns] = grads[rows, i * SIZE : (i + 1) * SIZE]

        @pl.when(r == q)
        def _(d=d):
            d[slot] = dt[...]

    @pl.when((turn == 0) & (part >= 1))
    def _():
        pair(part - 1, 1)

    @pl.when(turn == 1)
    def _():
        give(part, 0)

    @pl.when((turn == 1) & (part >= 2))
    def _():
        finish(part - 2)

    @pl.when(turn == 2)
    def _():
        pair(part, 0)

    @pl.when(turn == 3)
    def _():
        give(part, 1)

    @pl.when((turn == 3) & (part >= 2))
    def _():
        for copy in out(part - 2, lax.rem(part - 2, SLOTS)):
            copy.wait()

    @pl.when(t == STEPS - 1)
    def _():
        pair(part, 1)
        finish(part - 1)
        finish(part)
        for n, peer in enumerate((core_peer, x_peer)):
            copy = remote(sq.at[2 * n], sq.at[2 * n + 1], sq_send.at[n], sq_recv.at[n], peer)
            copy.start()
            copy.wait()
            if n == 0:
                sq[2] = sq[0] + sq[1]
            else:
                squares[...] = sq[2] + sq[3]
        for p in (part - 1, part):
            for copy in out(p, lax.rem(p, SLOTS)):
                copy.wait()


def backward(h1, a0, a0t, a1, a1t, dy, dyt, wg, wu, wd):
    wide = DP * SIZE
    row, col, vm, dma = (TOKENS, D), (D, TOKENS), pltpu.VMEM, pltpu.SemaphoreType.DMA
    gu, d = (SLOTS, 2, ROWS, wide), (SLOTS, SIZE, D)
    two_gu, two_d = (SLOTS, 2, 2, ROWS, wide), (SLOTS, 2, SIZE, D)
    return pl.pallas_call(
        backward_kernel,
        grid=(STEPS,),
        in_specs=[pl.BlockSpec(memory_space=pl.ANY)] * 10,
        out_specs=[pl.BlockSpec(memory_space=pl.ANY)] * 2 + [pl.BlockSpec((8, D), lambda t: (0, 0))],
        out_shape=[
            jax.ShapeDtypeStruct((LAYERS * PARTS, 2, ROWS, wide), BF16),
            jax.ShapeDtypeStruct((LAYERS * PARTS, SIZE, D), BF16),
            jax.ShapeDtypeStruct((8, D), F32),
        ],
        scratch_shapes=[
            *(vm(shape, BF16) for shape in (row, col, row, col, row)),
            vm(row, F32),
            *(vm(shape, BF16) for shape in ((2, D, 2 * SIZE), (2, SIZE, D), (TOKENS, SIZE), (TOKENS, 2 * SIZE), (SIZE, D), (D, 2 * SIZE))),
            *(vm(shape, BF16) for shape in (gu, gu, two_gu, two_gu, gu, d, d, two_d, two_d, d)),
            vm((4, 8, D), F32),
            dma((2, 3)),
            dma((5,)),
            *[dma((SLOTS, 2, 2))] * 4,
            dma((SLOTS, 2)),
            dma((2,)),
            dma((2,)),
            pltpu.SemaphoreType.REGULAR,
            pltpu.SemaphoreType.REGULAR,
        ],
        compiler_params=pltpu.CompilerParams(
            dimension_semantics=("arbitrary",), vmem_limit_bytes=VMEM, collective_id=0, has_side_effects=True
        ),
        cost_estimate=cost(14, 120e6),
        name="backward",
    )(h1, a0, a0t, a1, a1t, dy, dyt, wg, wu, wd)


def adamw_kernel(me_ref, f_ref, ggu, gd, wg, wu, wd, mg, mu, md, vg, vu, vd, *refs):
    ngu, nd, *mv = refs[-8:]
    factor = jnp.minimum(1.0, 0.5 * lax.rsqrt(jnp.sum(f_ref[...], keepdims=True) / COUNT + 1e-30))
    for k, (g, w, m, v, to) in enumerate(
        (
            (jnp.concatenate([ggu[p, 0] for p in range(ggu.shape[0])], 1), wg.at[0], mg.at[0], vg.at[0], ngu.at[0]),
            (jnp.concatenate([ggu[p, 1] for p in range(ggu.shape[0])], 1), wu.at[0], mu.at[0], vu.at[0], ngu.at[1]),
            (gd[...], wd.at[0], md.at[0], vd.at[0], nd),
        )
    ):
        g = g.astype(F32) * factor
        m = 0.9 * m[...] + 0.1 * g
        v = 0.95 * v[...] + 0.05 * g * g
        w = w[...].astype(F32)
        to[...] = (w - 0.02 * (m * lax.rsqrt(v + 1e-8) + 0.1 * w)).astype(BF16)
        mv[k][0] = m
        mv[3 + k][0] = v


def adamw(chunk, me, squares, ggu, gd, weights, m, v, so_far):
    layer, start, size = chunk
    step = size // DP
    w_spec = pl.BlockSpec((1, ROWS, size), lambda o, me: (layer, me[0], (o * OWN + start) // size))
    wd_spec = pl.BlockSpec((1, step, D), lambda o, me: (layer, (me[0] * OWN + start) // step + o, 0))
    mv_spec = pl.BlockSpec((1, ROWS, size), lambda o, me: (layer, 0, (o * OWN + start) // size))
    mvd_spec = pl.BlockSpec((1, step, D), lambda o, me: (layer, start // step + o, 0))
    gu_spec = pl.BlockSpec((2, ROWS, size), lambda o, me: (0, 0, o))
    d_spec = pl.BlockSpec((step, D), lambda o, me: (o, 0))
    part, parts = (1 - layer) * PARTS + start // SIZE, size // SIZE
    ggu_spec = pl.BlockSpec((parts, 2, ROWS, SIZE), lambda o, me: (part // parts, 0, 0, o))
    gd_spec = pl.BlockSpec((step, D), lambda o, me: (part * SIZE // step + o, 0))
    mv_specs = [mv_spec, mv_spec, mvd_spec] * 2
    return pl.pallas_call(
        adamw_kernel,
        grid_spec=pltpu.PrefetchScalarGridSpec(
            num_scalar_prefetch=1,
            grid=(DP,),
            in_specs=[whole((8, D)), ggu_spec, gd_spec, w_spec, w_spec, wd_spec, *mv_specs]
            + [pl.BlockSpec(memory_space=pl.ANY)] * len(so_far),
            out_specs=[gu_spec, d_spec, *mv_specs],
        ),
        out_shape=[jax.ShapeDtypeStruct((2, ROWS, DP * size), BF16), jax.ShapeDtypeStruct((size, D), BF16)]
        + [jax.ShapeDtypeStruct(t.shape, F32) for t in (*m, *v)],
        input_output_aliases={13 + n: 2 + n for n in range(len(so_far))},
        compiler_params=params(1),
        cost_estimate=cost(0.25, 17e6),
        name="adamw",
    )(me, squares, ggu, gd, *weights, *m, *v, *so_far)


def assemble_kernel(owners, me_ref, *refs):
    wg, wu, wd = refs[-3:]
    for q, (gu, d) in enumerate(zip(refs[0 : 2 * owners : 2], refs[1 : 2 * owners : 2])):

        @pl.when(pl.program_id(0) == q)
        def _(gu=gu, d=d):
            wg[0] = gu[0]
            wu[0] = gu[1]
            wd[0] = d[...]


def assemble(chunk, base, me, blocks, so_far):
    layer, start, size = chunk
    step = size // DP

    def when(q, r, o):
        return jnp.where(r == q, o, 0 if q else DP - 1)

    def gu_spec(q):
        return pl.BlockSpec((2, ROWS, size), lambda r, o, me: (0, 0, when(q, r, o)))

    def d_spec(q):
        return pl.BlockSpec((step, D), lambda r, o, me: (when(q, r, o), 0))

    def owner(r, me):
        return (r + base) ^ me[0]

    w_spec = pl.BlockSpec((1, ROWS, size), lambda r, o, me: (layer, owner(r, me), (o * OWN + start) // size))
    wd_spec = pl.BlockSpec((1, step, D), lambda r, o, me: (layer, (owner(r, me) * OWN + start) // step + o, 0))
    wide, tall = jax.ShapeDtypeStruct((LAYERS, D, FF), BF16), jax.ShapeDtypeStruct((LAYERS, FF, D), BF16)
    return pl.pallas_call(
        functools.partial(assemble_kernel, len(blocks)),
        grid_spec=pltpu.PrefetchScalarGridSpec(
            num_scalar_prefetch=1,
            grid=(len(blocks), DP),
            in_specs=[spec(q) for q in range(len(blocks)) for spec in (gu_spec, d_spec)] + [pl.BlockSpec(memory_space=pl.ANY)] * len(so_far),
            out_specs=[w_spec, w_spec, wd_spec],
        ),
        out_shape=[wide, wide, tall],
        input_output_aliases={1 + 2 * len(blocks) + n: n for n in range(len(so_far))},
        compiler_params=params(2),
        cost_estimate=cost(0.15, 6e6),
        name="assemble",
    )(me, *(t for block in blocks for t in block), *so_far)


def to_core(t):
    return lax.ppermute(t, "dp", [(0, 1), (1, 0), (2, 3), (3, 2)])


def to_x(t):
    return lax.ppermute(t, "dp", [(0, 2), (2, 0), (1, 3), (3, 1)])


def solution(mesh):
    def body(x, dy, *arrays):
        weights, m, v = (arrays[i : i + 3] for i in (0, 3, 6))
        x, dy = x[0], dy[0]
        me = lax.axis_index("dp").astype(jnp.int32)[None]

        h1, a0, a1, a0t, a1t, dyt = forward(x, dy, *weights)

        gu, d, squares = backward(h1, a0, a0t, a1, a1t, dy, dyt, *weights)
        d = d.reshape(-1, D)

        moments, own, near, far, last, new = (), {}, {}, {}, {}, ()
        turn = [LAST - 1, *range(LAST - 1), LAST]
        for n, k in enumerate(turn):
            own_gu, own_d, *moments = adamw(CHUNKS[k], me, squares, gu, d, weights, m, v, moments)
            own[n] = own_gu, own_d
            far[n] = tuple(map(to_x, own[n]))
            near[n] = tuple(map(to_core, own[n]))
            last[n] = tuple(map(to_core, far[n]))
        for n in range(LAST + 1):
            for ahead in (0, 1, 2) if n == 0 else (n + 2,):
                if ahead <= LAST:
                    new = assemble(CHUNKS[turn[ahead]], 0, me, (own[ahead], near[ahead]), new)
            for base, blocks in ((2, (far[n],)), (3, (last[n],))) if n == LAST else ((2, (far[n], last[n])),):
                new = assemble(CHUNKS[turn[n]], base, me, blocks, new)
        return (*new, *moments)

    rows = P(None, "dp", None)
    return jax.shard_map(
        body,
        mesh=mesh,
        in_specs=(P(("rep", "dp"), None, None),) * 2 + (P(None, None, None),) * 3 + (rows,) * 6,
        out_specs=(P("rep", None, None),) * 3 + (P("rep", "dp", None),) * 6,
        check_vma=False,
    )
```

```python
import functools

import jax
import jax.numpy as jnp
from jax import lax
from jax.experimental import pallas as pl
from jax.experimental.pallas import tpu as pltpu
from jax.sharding import PartitionSpec as P


F32, BF16 = jnp.float32, jnp.bfloat16
TOKENS, D, FF = 2048, 512, 8192
LAYERS, DP = 2, 4
OWN = FF // DP
SIZE = 256
PARTS = OWN // SIZE
STEPS = LAYERS * PARTS * DP
SLOTS = 3
CHUNKS = [(1, start, 512) for start in range(0, OWN, 512)] + [(0, 0, 512), (0, 512, 512), (0, 1024, 512), (0, 1536, 256), (0, 1792, 256)]
LAST = len(CHUNKS) - 1
ROWS = D // DP
COUNT = 3 * LAYERS * D * FF
VMEM = 60 * 1024 * 1024


def dot(a, b):
    return jnp.dot(a, b, preferred_element_type=F32)


def dot_nt(a, b):
    return lax.dot_general(a, b, (((1,), (1,)), ((), ())), preferred_element_type=F32)


def sigmoid(x):
    return 0.5 * jnp.tanh(0.5 * x) + 0.5


def normed(h):
    wide = h.astype(F32)
    return (wide * lax.rsqrt(jnp.mean(wide * wide, -1, keepdims=True) + 1e-6)).astype(BF16)


def flipped(t):
    return t.astype(F32).T.astype(BF16)


def whole(shape):
    return pl.BlockSpec(shape, lambda *_: (0,) * len(shape), pipeline_mode=pl.Buffered(1))


def params(n):
    return pltpu.CompilerParams(dimension_semantics=("arbitrary",) * n, vmem_limit_bytes=VMEM)


def cost(units, moved):
    return pl.CostEstimate(flops=int(units * 2 * TOKENS * D * FF), bytes_accessed=int(moved), transcendentals=0)


FT, FI = 1024, 2048


def forward_kernel(x_ref, wg_ref, wu_ref, wd_ref, h1_ref, a0_ref, a1_ref, a0t_ref, a1t_ref, acc_ref, z_ref):
    j, i = pl.program_id(0), pl.program_id(1)
    rows = pl.ds(pl.multiple_of(i * FI, FI), FI)

    @pl.when(j == 0)
    def _():
        a = normed(x_ref[rows, :])
        a0_ref[rows, :] = a
        a0t_ref[:, rows] = flipped(a)
        acc_ref[rows, :] = jnp.zeros((FI, D), F32)

    a = a0_ref[rows, :]
    for s in range(0, FT, 256):
        gate = dot(a, wg_ref[0, :, s : s + 256])
        up = dot(a, wu_ref[0, :, s : s + 256])
        z_ref[:, s : s + 256] = (gate * sigmoid(gate) * up).astype(BF16)
    acc_ref[rows, :] += dot(z_ref[...], wd_ref[0])

    @pl.when(j == FF // FT - 1)
    def _():
        h1 = x_ref[rows, :] + acc_ref[rows, :].astype(BF16)
        a1 = normed(h1)
        h1_ref[rows, :] = h1
        a1_ref[rows, :] = a1
        a1t_ref[:, rows] = flipped(a1)


def forward(x, wg, wu, wd):
    row, col = jax.ShapeDtypeStruct((TOKENS, D), BF16), jax.ShapeDtypeStruct((D, TOKENS), BF16)
    return pl.pallas_call(
        forward_kernel,
        grid=(FF // FT, TOKENS // FI),
        in_specs=[
            whole((TOKENS, D)),
            pl.BlockSpec((1, D, FT), lambda j, i: (0, 0, j)),
            pl.BlockSpec((1, D, FT), lambda j, i: (0, 0, j)),
            pl.BlockSpec((1, FT, D), lambda j, i: (0, j, 0)),
        ],
        out_specs=[whole((TOKENS, D))] * 3 + [whole((D, TOKENS))] * 2,
        out_shape=[row] * 3 + [col] * 2,
        scratch_shapes=[pltpu.VMEM((TOKENS, D), F32), pltpu.VMEM((FI, FT), BF16)],
        compiler_params=params(2),
        cost_estimate=cost(3, 40e6),
        name="forward0",
    )(x, wg, wu, wd)


BI = 512


def backward_kernel(
    h1, a0, a0t, a1, a1t, dy0, wg, wu, wd, gu_out, d_out, squares,
    a, at, dy, dyt, h, da, wgu_buf, wd_buf, z, dgu, dt, grads,
    own_gu, far_gu, give_gu, core_gu, x_gu, own_d, far_d, give_d, core_d, x_d, sq,
    w_sem, in_sem, core_send, core_recv, x_send, x_recv, out_sem, sq_send, sq_recv, core_free, x_free,
):
    t = pl.program_id(0)
    part, turn = lax.div(t, DP), lax.rem(t, DP)
    r = lax.rem(turn + 2, DP)
    slot = lax.rem(part, SLOTS)
    rep, me = lax.axis_index("rep"), lax.axis_index("dp")
    mx, mc = lax.div(me, 2), lax.rem(me, 2)

    def related(qx, qc):
        return lax.rem(mx + qx, 2) * 2 + lax.rem(mc + qc, 2)

    core_peer, x_peer = (rep, related(0, 1)), (rep, related(1, 0))
    mesh_id = pl.DeviceIdType.MESH

    def weights(t):
        part, r = lax.div(t, DP), lax.rem(t + 2, DP)
        layer = 1 - lax.div(part, PARTS)
        at_ff = pl.multiple_of(related(lax.div(r, 2), lax.rem(r, 2)) * OWN + lax.rem(part, PARTS) * SIZE, SIZE)
        n = lax.rem(t, 2)
        return (
            pltpu.make_async_copy(wg.at[layer, :, pl.ds(at_ff, SIZE)], wgu_buf.at[n, :, 0:SIZE], w_sem.at[n, 0]),
            pltpu.make_async_copy(wu.at[layer, :, pl.ds(at_ff, SIZE)], wgu_buf.at[n, :, SIZE : 2 * SIZE], w_sem.at[n, 1]),
            pltpu.make_async_copy(wd.at[layer, pl.ds(at_ff, SIZE), :], wd_buf.at[n], w_sem.at[n, 2]),
        )

    def inputs(*sources):
        pairs = zip(sources, (a, at, dy, h))
        return [pltpu.make_async_copy(src, dst, in_sem.at[n]) for n, (src, dst) in enumerate(pairs)]

    def columns_of(half):
        return pl.ds(pl.multiple_of((mx if half else 1 - mx) * 2 * SIZE, 2 * SIZE), 2 * SIZE)

    def remote(src, dst, send, recv, peer):
        return pltpu.make_async_remote_copy(src, dst, send, recv, device_id=peer, device_id_type=mesh_id)

    def to_core(n, half):
        c = columns_of(half)
        pairs = ((give_gu.at[n, :, :, :, c], core_gu.at[n, :, :, :, c]), (give_d.at[n, 1 - half], core_d.at[n, 1 - half]))
        return [remote(src, dst, core_send.at[n, half, i], core_recv.at[n, half, i], core_peer) for i, (src, dst) in enumerate(pairs)]

    def to_x(n, half):
        c = columns_of(half)
        pairs = ((far_gu.at[n, :, :, c], x_gu.at[n, :, :, c]), (far_d.at[n], x_d.at[n]))[: 2 - half]
        return [remote(src, dst, x_send.at[n, half, i], x_recv.at[n, half, i], x_peer) for i, (src, dst) in enumerate(pairs)]

    def out(p, n):
        return [
            pltpu.make_async_copy(src.at[n], dst.at[p], out_sem.at[n, i]) for i, (src, dst) in enumerate(((own_gu, gu_out), (own_d, d_out)))
        ]

    def give(p, half):
        n = lax.rem(p, SLOTS)
        if half == 0:

            @pl.when(p >= SLOTS)
            def _():
                pl.semaphore_wait(core_free, 1)

        for copy in to_core(n, half):
            copy.start()

    def pair(p, half):
        n = lax.rem(p, SLOTS)
        for copy in to_core(n, half):
            copy.wait_recv()
        c = columns_of(half)
        far_gu[n, :, :, c] = (far_gu[n, :, :, c].astype(F32) + core_gu[n, 1, :, :, c].astype(F32)).astype(BF16)
        if half == 0:
            far_d[n] = (far_d[n].astype(F32) + core_d[n, 1].astype(F32)).astype(BF16)

            @pl.when(p >= SLOTS)
            def _():
                pl.semaphore_wait(x_free, 1)

        for copy in to_x(n, half):
            copy.start()

    def finish(p):
        n = lax.rem(p, SLOTS)
        for half in range(2):
            for copy in to_x(n, half):
                copy.wait()
            for copy in to_core(n, half):
                copy.wait_send()
        total = (own_gu[n].astype(F32) + core_gu[n, 0].astype(F32) + x_gu[n].astype(F32)).astype(BF16)
        own_gu[n] = total
        total = total.astype(F32)
        line = jnp.sum(total[0] * total[0] + total[1] * total[1], 0, keepdims=True)
        line = sum(line[:, i : i + D] for i in range(0, line.shape[1], D))
        total = (own_d[n].astype(F32) + core_d[n, 0].astype(F32) + x_d[n].astype(F32)).astype(BF16)
        own_d[n] = total
        total = total.astype(F32)
        sq[0, 0:1, :] += line + jnp.sum(total * total, 0, keepdims=True)

        @pl.when(p < LAYERS * PARTS - SLOTS)
        def _():
            pl.semaphore_signal(core_free, inc=1, device_id=core_peer, device_id_type=mesh_id)
            pl.semaphore_signal(x_free, inc=1, device_id=x_peer, device_id_type=mesh_id)

        for copy in out(p, n):
            copy.start()

    @pl.when(t == 0)
    def _():
        barrier = pltpu.get_barrier_semaphore()
        for peer in (core_peer, x_peer):
            pl.semaphore_signal(barrier, inc=1, device_id=peer, device_id_type=mesh_id)
        for copy in (*weights(t), *inputs(a1, a1t, dy0, h1)):
            copy.start()
        da[...] = jnp.zeros_like(da)
        sq[...] = jnp.zeros_like(sq)
        for copy in inputs(a1, a1t, dy0, h1):
            copy.wait()
        for b in range(0, TOKENS, BI):
            rows = slice(b, b + BI)
            dyt[:, rows] = flipped(dy[rows, :])
        pl.semaphore_wait(barrier, 2)

    for copy in weights(t):
        copy.wait()

    @pl.when(t < STEPS - 1)
    def _():
        for copy in weights(t + 1):
            copy.start()

    @pl.when(t == STEPS // 2)
    def _():
        for copy in inputs(a0, a0t):
            copy.start()
        for b in range(0, TOKENS, BI):
            rows = slice(b, b + BI)
            back = da[rows, :].astype(BF16).astype(F32)
            wide = h[rows, :].astype(F32)
            scale = lax.rsqrt(jnp.mean(wide * wide, -1, keepdims=True) + 1e-6)
            along = jnp.mean(back * wide, -1, keepdims=True)
            dh = dy[rows, :] + (back * scale - wide * (scale * scale * scale * along)).astype(BF16)
            dy[rows, :] = dh
            dyt[:, rows] = flipped(dh)
        for copy in inputs(a0, a0t):
            copy.wait()

    def tile(with_da):
        w = lax.rem(t, 2)
        for b in range(0, TOKENS, BI):
            rows = slice(b, b + BI)
            both = dot(a[rows, :], wgu_buf[w])
            gate, up = both[:, :SIZE], both[:, SIZE:]
            dz = dot_nt(dy[rows, :], wd_buf[w]).astype(BF16).astype(F32)
            sig = sigmoid(gate)
            act = gate * sig
            z[rows, :] = (act * up).astype(BF16)
            dgu[rows, SIZE : 2 * SIZE] = (dz * act).astype(BF16)
            dgu[rows, 0:SIZE] = (dz * up * (sig + act * (1.0 - sig))).astype(BF16)
        dt[...] = dot(dyt[...], z[...]).T.astype(BF16)
        grads[...] = dot(at[...], dgu[...]).astype(BF16)
        if with_da:
            for b in range(0, TOKENS, BI):
                rows = slice(b, b + BI)
                da[rows, :] += dot_nt(dgu[rows, :], wgu_buf[w])

    @pl.when(t < STEPS // 2)
    def _():
        tile(True)

    @pl.when(t >= STEPS // 2)
    def _():
        tile(False)

    columns = pl.ds(pl.multiple_of(related(lax.div(r, 2), lax.rem(r, 2)) * SIZE, SIZE), SIZE)
    for q, (gu, d) in enumerate(((own_gu, own_d), (give_gu.at[:, 0], give_d.at[:, 0]), (far_gu, far_d), (give_gu.at[:, 1], give_d.at[:, 1]))):
        rows = pl.ds(pl.multiple_of(related(q // 2, q % 2) * ROWS, ROWS), ROWS)
        for i in range(2):
            gu[slot, i, :, columns] = grads[rows, i * SIZE : (i + 1) * SIZE]

        @pl.when(r == q)
        def _(d=d):
            d[slot] = dt[...]

    @pl.when((turn == 0) & (part >= 1))
    def _():
        pair(part - 1, 1)

    @pl.when(turn == 1)
    def _():
        give(part, 0)

    @pl.when((turn == 1) & (part >= 2))
    def _():
        finish(part - 2)

    @pl.when(turn == 2)
    def _():
        pair(part, 0)

    @pl.when(turn == 3)
    def _():
        give(part, 1)

    @pl.when((turn == 3) & (part >= 2))
    def _():
        for copy in out(part - 2, lax.rem(part - 2, SLOTS)):
            copy.wait()

    @pl.when(t == STEPS - 1)
    def _():
        pair(part, 1)
        finish(part - 1)
        finish(part)
        for n, peer in enumerate((core_peer, x_peer)):
            copy = remote(sq.at[2 * n], sq.at[2 * n + 1], sq_send.at[n], sq_recv.at[n], peer)
            copy.start()
            copy.wait()
            if n == 0:
                sq[2] = sq[0] + sq[1]
            else:
                squares[...] = sq[2] + sq[3]
        for p in (part - 1, part):
            for copy in out(p, lax.rem(p, SLOTS)):
                copy.wait()


def backward(h1, a0, a0t, a1, a1t, dy, wg, wu, wd):
    wide = DP * SIZE
    row, col, vm, dma = (TOKENS, D), (D, TOKENS), pltpu.VMEM, pltpu.SemaphoreType.DMA
    gu, d = (SLOTS, 2, ROWS, wide), (SLOTS, SIZE, D)
    two_gu, two_d = (SLOTS, 2, 2, ROWS, wide), (SLOTS, 2, SIZE, D)
    return pl.pallas_call(
        backward_kernel,
        grid=(STEPS,),
        in_specs=[pl.BlockSpec(memory_space=pl.ANY)] * 9,
        out_specs=[pl.BlockSpec(memory_space=pl.ANY)] * 2 + [pl.BlockSpec((8, D), lambda t: (0, 0))],
        out_shape=[
            jax.ShapeDtypeStruct((LAYERS * PARTS, 2, ROWS, wide), BF16),
            jax.ShapeDtypeStruct((LAYERS * PARTS, SIZE, D), BF16),
            jax.ShapeDtypeStruct((8, D), F32),
        ],
        scratch_shapes=[
            *(vm(shape, BF16) for shape in (row, col, row, col, row)),
            vm(row, F32),
            *(vm(shape, BF16) for shape in ((2, D, 2 * SIZE), (2, SIZE, D), (TOKENS, SIZE), (TOKENS, 2 * SIZE), (SIZE, D), (D, 2 * SIZE))),
            *(vm(shape, BF16) for shape in (gu, gu, two_gu, two_gu, gu, d, d, two_d, two_d, d)),
            vm((4, 8, D), F32),
            dma((2, 3)),
            dma((5,)),
            *[dma((SLOTS, 2, 2))] * 4,
            dma((SLOTS, 2)),
            dma((2,)),
            dma((2,)),
            pltpu.SemaphoreType.REGULAR,
            pltpu.SemaphoreType.REGULAR,
        ],
        compiler_params=pltpu.CompilerParams(
            dimension_semantics=("arbitrary",), vmem_limit_bytes=VMEM, collective_id=0, has_side_effects=True
        ),
        cost_estimate=cost(14, 120e6),
        name="backward",
    )(h1, a0, a0t, a1, a1t, dy, wg, wu, wd)


def adamw_kernel(me_ref, f_ref, ggu, gd, wg, wu, wd, mg, mu, md, vg, vu, vd, *refs):
    ngu, nd, *mv = refs[-8:]
    factor = jnp.minimum(1.0, 0.5 * lax.rsqrt(jnp.sum(f_ref[...], keepdims=True) / COUNT + 1e-30))
    for k, (g, w, m, v, to) in enumerate(
        (
            (jnp.concatenate([ggu[p, 0] for p in range(ggu.shape[0])], 1), wg.at[0], mg.at[0], vg.at[0], ngu.at[0]),
            (jnp.concatenate([ggu[p, 1] for p in range(ggu.shape[0])], 1), wu.at[0], mu.at[0], vu.at[0], ngu.at[1]),
            (gd[...], wd.at[0], md.at[0], vd.at[0], nd),
        )
    ):
        g = g.astype(F32) * factor
        m = 0.9 * m[...] + 0.1 * g
        v = 0.95 * v[...] + 0.05 * g * g
        w = w[...].astype(F32)
        to[...] = (w - 0.02 * (m * lax.rsqrt(v + 1e-8) + 0.1 * w)).astype(BF16)
        mv[k][0] = m
        mv[3 + k][0] = v


def adamw(chunk, me, squares, ggu, gd, weights, m, v, so_far):
    layer, start, size = chunk
    step = size // DP
    w_spec = pl.BlockSpec((1, ROWS, size), lambda o, me: (layer, me[0], (o * OWN + start) // size))
    wd_spec = pl.BlockSpec((1, step, D), lambda o, me: (layer, (me[0] * OWN + start) // step + o, 0))
    mv_spec = pl.BlockSpec((1, ROWS, size), lambda o, me: (layer, 0, (o * OWN + start) // size))
    mvd_spec = pl.BlockSpec((1, step, D), lambda o, me: (layer, start // step + o, 0))
    gu_spec = pl.BlockSpec((2, ROWS, size), lambda o, me: (0, 0, o))
    d_spec = pl.BlockSpec((step, D), lambda o, me: (o, 0))
    part, parts = (1 - layer) * PARTS + start // SIZE, size // SIZE
    ggu_spec = pl.BlockSpec((parts, 2, ROWS, SIZE), lambda o, me: (part // parts, 0, 0, o))
    gd_spec = pl.BlockSpec((step, D), lambda o, me: (part * SIZE // step + o, 0))
    mv_specs = [mv_spec, mv_spec, mvd_spec] * 2
    return pl.pallas_call(
        adamw_kernel,
        grid_spec=pltpu.PrefetchScalarGridSpec(
            num_scalar_prefetch=1,
            grid=(DP,),
            in_specs=[whole((8, D)), ggu_spec, gd_spec, w_spec, w_spec, wd_spec, *mv_specs]
            + [pl.BlockSpec(memory_space=pl.ANY)] * len(so_far),
            out_specs=[gu_spec, d_spec, *mv_specs],
        ),
        out_shape=[jax.ShapeDtypeStruct((2, ROWS, DP * size), BF16), jax.ShapeDtypeStruct((size, D), BF16)]
        + [jax.ShapeDtypeStruct(t.shape, F32) for t in (*m, *v)],
        input_output_aliases={13 + n: 2 + n for n in range(len(so_far))},
        compiler_params=params(1),
        cost_estimate=cost(0.25, 17e6),
        name="adamw",
    )(me, squares, ggu, gd, *weights, *m, *v, *so_far)


def assemble_kernel(owners, me_ref, *refs):
    wg, wu, wd = refs[-3:]
    for q, (gu, d) in enumerate(zip(refs[0 : 2 * owners : 2], refs[1 : 2 * owners : 2])):

        @pl.when(pl.program_id(0) == q)
        def _(gu=gu, d=d):
            wg[0] = gu[0]
            wu[0] = gu[1]
            wd[0] = d[...]


def assemble(chunk, base, me, blocks, so_far):
    layer, start, size = chunk
    step = size // DP

    def when(q, r, o):
        return jnp.where(r == q, o, 0 if q else DP - 1)

    def gu_spec(q):
        return pl.BlockSpec((2, ROWS, size), lambda r, o, me: (0, 0, when(q, r, o)))

    def d_spec(q):
        return pl.BlockSpec((step, D), lambda r, o, me: (when(q, r, o), 0))

    def owner(r, me):
        return (r + base) ^ me[0]

    w_spec = pl.BlockSpec((1, ROWS, size), lambda r, o, me: (layer, owner(r, me), (o * OWN + start) // size))
    wd_spec = pl.BlockSpec((1, step, D), lambda r, o, me: (layer, (owner(r, me) * OWN + start) // step + o, 0))
    wide, tall = jax.ShapeDtypeStruct((LAYERS, D, FF), BF16), jax.ShapeDtypeStruct((LAYERS, FF, D), BF16)
    return pl.pallas_call(
        functools.partial(assemble_kernel, len(blocks)),
        grid_spec=pltpu.PrefetchScalarGridSpec(
            num_scalar_prefetch=1,
            grid=(len(blocks), DP),
            in_specs=[spec(q) for q in range(len(blocks)) for spec in (gu_spec, d_spec)] + [pl.BlockSpec(memory_space=pl.ANY)] * len(so_far),
            out_specs=[w_spec, w_spec, wd_spec],
        ),
        out_shape=[wide, wide, tall],
        input_output_aliases={1 + 2 * len(blocks) + n: n for n in range(len(so_far))},
        compiler_params=params(2),
        cost_estimate=cost(0.15, 6e6),
        name="assemble",
    )(me, *(t for block in blocks for t in block), *so_far)


def to_core(t):
    return lax.ppermute(t, "dp", [(0, 1), (1, 0), (2, 3), (3, 2)])


def to_x(t):
    return lax.ppermute(t, "dp", [(0, 2), (2, 0), (1, 3), (3, 1)])


def solution(mesh):
    def body(x, dy, *arrays):
        weights, m, v = (arrays[i : i + 3] for i in (0, 3, 6))
        x, dy = x[0], dy[0]
        me = lax.axis_index("dp").astype(jnp.int32)[None]

        h1, a0, a1, a0t, a1t = forward(x, *weights)

        gu, d, squares = backward(h1, a0, a0t, a1, a1t, dy, *weights)
        d = d.reshape(-1, D)

        moments, own, near, far, last, new = (), {}, {}, {}, {}, ()
        turn = [LAST - 1, *range(LAST - 1), LAST]
        for n, k in enumerate(turn):
            own_gu, own_d, *moments = adamw(CHUNKS[k], me, squares, gu, d, weights, m, v, moments)
            own[n] = own_gu, own_d
            far[n] = tuple(map(to_x, own[n]))
            near[n] = tuple(map(to_core, own[n]))
            last[n] = tuple(map(to_core, far[n]))
        for n in range(LAST + 1):
            for ahead in (0, 1, 2) if n == 0 else (n + 2,):
                if ahead <= LAST:
                    new = assemble(CHUNKS[turn[ahead]], 0, me, (own[ahead], near[ahead]), new)
            for base, blocks in ((2, (far[n],)), (3, (last[n],))) if n == LAST else ((2, (far[n], last[n])),):
                new = assemble(CHUNKS[turn[n]], base, me, blocks, new)
        return (*new, *moments)

    rows = P(None, "dp", None)
    return jax.shard_map(
        body,
        mesh=mesh,
        in_specs=(P(("rep", "dp"), None, None),) * 2 + (P(None, None, None),) * 3 + (rows,) * 6,
        out_specs=(P("rep", None, None),) * 3 + (P("rep", "dp", None),) * 6,
        check_vma=False,
    )
```
